32 devices in a mesh: groups: 2 (over x), ctx: 16 (over z, y, core).
Axes of the slice: x: 2, y: 2, z: 4, core: 2. Of those that a mesh axis runs over, the one named last changes fastest.
Arguments:
- queries: bfloat16 [8192, 1024], P(('groups', 'ctx')), parts along dimension 0, may hold values from -7 to 7
- keys: bfloat16 [8192, 128], P(('groups', 'ctx')), parts along dimension 0, may hold values from -7 to 7
- values: bfloat16 [8192, 128], P(('groups', 'ctx')), parts along dimension 0, may hold values from -6 to 6
- span_order: int32 [64], P('groups'), parts along dimension 0, may hold values from 0 to 31, as said below
Outputs:
- attended: bfloat16 [8192, 1024], P(('groups', 'ctx')), parts along dimension 0
The draws below stay inside these ranges and needn't reach their ends.
There are 2 independent parts, one for each index of `groups`. The reference program is written for one: setup_inputs(seed, part) draws one part's arguments, and reference() takes and returns one part's arrays. A program takes and returns all parts, laid end to end along the dimension named above; each array names one. Nothing has to cross between parts.
Inputs may be any that keep to these rules, and one draw needn't show every extreme that they name: A permutation: rows j * 128 to (j + 1) * 128 - 1 hold span span_order[j] of the sequence; for every j, span_order[2 j] + span_order[2 j + 1] = 31.
All inputs are finite; a program needn't handle non-finite values.
Results may differ from the reference program's by a relative error of at most 0.006.
Values may be sent and summed in bfloat16 or wider, within the bound.
A program may use at most 64 MiB of HBM per device.

```python
import math
import jax
import jax.numpy as jnp
from jax import lax

QH = 8
DH = 128
SPAN = 128
SEQ = 4096
NSPAN = 32


def drawn_pair(key):
    query_key = jax.random.fold_in(key, 11)
    keys_key = jax.random.fold_in(key, 12)
    query_draw = jnp.clip(jax.random.normal(query_key, (SEQ, QH * DH), jnp.float32), -5.0, 5.0)
    keys_draw = jnp.clip(jax.random.normal(keys_key, (SEQ, DH), jnp.float32), -5.0, 5.0)
    return (query_draw, keys_draw)


def draw_queries(key, part):
    return drawn_pair(key)[0].astype(jnp.bfloat16)


def draw_keys(key, part):
    return drawn_pair(key)[1].astype(jnp.bfloat16)


def draw_span_order(key, part):
    half = NSPAN // 2
    pairs = jax.random.permutation(jax.random.fold_in(key, 21), half).astype(jnp.int32)
    flipped = jax.random.randint(jax.random.fold_in(key, 22), (half,), 0, 2)
    early = pairs
    late = (NSPAN - 1 - pairs).astype(jnp.int32)
    first = jnp.where(flipped == 1, late, early)
    second = jnp.where(flipped == 1, early, late)
    return jnp.stack([first, second], axis=1).reshape(NSPAN).astype(jnp.int32)


def shard_levels(stream_key, shape, cuts, smallest, top_value):
    factor_of = 1.0
    for dim, parts in cuts:
        draws = jax.random.uniform(jax.random.fold_in(jax.random.fold_in(stream_key, 6), dim), (parts,), jnp.float32, smallest / len(cuts), top_value / len(cuts))
        factor_of = factor_of * jnp.repeat(jnp.exp(draws), shape[dim] // parts).reshape((-1,) + (1,) * (len(shape) - 1 - dim))
    return factor_of


def noise(stream_key, shape, width, most, cuts=(), held_as=jnp.bfloat16):
    array = width * jax.random.normal(stream_key, shape, jnp.float32)
    if cuts:
        array = array * shard_levels(stream_key, shape, cuts, -0.22, 0.18)
    return jnp.clip(array, -most, most).astype(held_as)


def setup_inputs(seed: int = 0, part: int = 0) -> dict:
    arg_keys = jax.random.split(jax.random.key(seed), 5)
    own_keys = jax.random.split(jax.random.fold_in(arg_keys[4], part), 5)
    return {
        "queries": draw_queries(jax.random.fold_in(jax.random.fold_in(arg_keys[4], part), 71), part),
        "keys": draw_keys(jax.random.fold_in(jax.random.fold_in(arg_keys[4], part), 71), part),
        "values": noise(own_keys[2], (SEQ, DH), 1.0, 6.0, ((0, 16),)),
        "span_order": draw_span_order(jax.random.fold_in(jax.random.fold_in(arg_keys[4], part), 71), part),
    }


def reference(queries, keys, values, span_order):
    total_rows = queries.shape[0]
    rows = jnp.arange(total_rows, dtype=jnp.int32)
    position = (span_order[rows // SPAN] * SPAN + rows % SPAN).astype(jnp.int32)
    block = math.gcd(total_rows, 512)
    scale = 1.0 / math.sqrt(DH)
    keys_f = keys.astype(jnp.float32)
    values_f = values.astype(jnp.float32)

    def one_block(index):
        first = (index * block).astype(jnp.int32)
        query_blk = lax.dynamic_slice_in_dim(queries, first, block, 0).reshape(block, QH, DH).astype(jnp.float32)
        query_pos = lax.dynamic_slice_in_dim(position, first, block, 0)
        score = jnp.einsum('qhd,kd->hqk', query_blk, keys_f) * scale
        kept = position[None, None, :] <= query_pos[None, :, None]
        score = jnp.where(kept, score, jnp.float32(-1e+30))
        top = lax.optimization_barrier(jnp.max(score, axis=-1, keepdims=True))
        weight = jnp.where(kept, jnp.exp(score - top), jnp.float32(0.0))
        total = lax.optimization_barrier(jnp.sum(weight, axis=-1))
        weight_b = lax.optimization_barrier(weight.astype(jnp.bfloat16)).astype(jnp.float32)
        mixed = jnp.einsum('hqk,kd->hqd', weight_b, values_f) / total[:, :, None]
        return jnp.transpose(mixed, (1, 0, 2)).reshape(block, QH * DH).astype(jnp.bfloat16)
    outputs = lax.map(one_block, jnp.arange(total_rows // block, dtype=jnp.int32))
    return outputs.reshape(total_rows, QH * DH)
```

```python
import functools
import math

import jax
import jax.numpy as jnp
from jax import lax
from jax.experimental import pallas as pl
from jax.experimental.pallas import tpu as pltpu
from jax.sharding import PartitionSpec as P

UP, DOWN, SIDE, TWIN = 0, 1, 2, 3
NEG = -1e30
FUSED_MOST = 32


def gather_kernel(n, k_ref, v_ref, buf, send_sem, recv_sem):
    lanes = 4
    zs = n // lanes
    me = lax.axis_index("ctx")
    z = me // lanes
    lane = lax.rem(me, lanes)
    y = lane // 2
    c = lax.rem(lane, 2)
    side = z * lanes + (1 - y) * 2 + c
    twin = z * lanes + y * 2 + (1 - c)
    not_top = z < zs - 1
    not_bottom = z > 0
    up = jnp.minimum(me + lanes, n - lanes + lane)
    down = jnp.maximum(me - lanes, lane)
    target = (up, down, side, twin)

    barrier = pltpu.get_barrier_semaphore()

    def greet(who):
        pl.semaphore_signal(
            barrier, inc=1, device_id={"ctx": who}, device_id_type=pl.DeviceIdType.MESH
        )

    greet(side)
    greet(twin)
    pl.when(not_top)(lambda: greet(up))
    pl.when(not_bottom)(lambda: greet(down))
    pl.semaphore_wait(barrier, 2 + not_top.astype(jnp.int32) + not_bottom.astype(jnp.int32))

    def copy(block, kv, route, src=None):
        return pltpu.make_async_remote_copy(
            src_ref=buf.at[block, kv] if src is None else src,
            dst_ref=buf.at[block, kv],
            send_sem=send_sem.at[block, kv, route],
            recv_sem=recv_sem.at[block, kv],
            device_id={"ctx": target[route]},
            device_id_type=pl.DeviceIdType.MESH,
        )

    own = (k_ref, v_ref)
    for kv in range(2):
        pl.when(not_top)(lambda: copy(me, kv, UP, own[kv]).start())
        pl.when(not_bottom)(lambda: copy(me, kv, DOWN, own[kv]).start())
        copy(me, kv, SIDE, own[kv]).start()
        copy(me, kv, TWIN, own[kv]).start()
    buf[me, 0] = k_ref[...]
    buf[me, 1] = v_ref[...]

    def at(zz, yy, cc):
        return zz * lanes + yy * 2 + cc

    def from_line(zz, onward, keep):
        block = at(zz, y, c)
        for kv in range(2):
            copy(block, kv, onward).wait_recv()
            pl.when(keep)(lambda: copy(block, kv, onward).start())
            copy(block, kv, SIDE).start()
            copy(block, kv, TWIN).start()

    def from_side(zz):
        block = at(zz, 1 - y, c)
        for kv in range(2):
            copy(block, kv, TWIN).wait_recv()
            copy(block, kv, TWIN).start()

    def from_twin(zz):
        for yy in (y, 1 - y):
            for kv in range(2):
                copy(at(zz, yy, 1 - c), kv, TWIN).wait_recv()

    def both(s, low, high):
        pl.when(z >= s)(lambda: low(z - s))
        pl.when(z + s < zs)(lambda: high(z + s))

    for s in range(1, zs):
        both(s, lambda zz: from_line(zz, UP, not_top), lambda zz: from_line(zz, DOWN, not_bottom))
        if s == 1:
            from_side(z)
        else:
            both(s - 1, from_side, from_side)
    both(zs - 1, from_side, from_side)
    from_twin(z)
    for s in range(1, zs):
        both(s, from_twin, from_twin)

    for kv in range(2):
        pl.when(not_top)(lambda: copy(me, kv, UP, own[kv]).wait_send())
        pl.when(not_bottom)(lambda: copy(me, kv, DOWN, own[kv]).wait_send())
        copy(me, kv, SIDE, own[kv]).wait_send()
        copy(me, kv, TWIN, own[kv]).wait_send()

    def line_sent(zz, onward, keep):
        for kv in range(2):
            pl.when(keep)(lambda: copy(at(zz, y, c), kv, onward).wait_send())
            copy(at(zz, y, c), kv, SIDE).wait_send()
            copy(at(zz, y, c), kv, TWIN).wait_send()

    def side_sent(zz):
        for kv in range(2):
            copy(at(zz, 1 - y, c), kv, TWIN).wait_send()

    side_sent(z)
    for s in range(1, zs):
        both(s, lambda zz: line_sent(zz, UP, not_top), lambda zz: line_sent(zz, DOWN, not_bottom))
        both(s, side_sent, side_sent)


def attend_kernel(
    n, heads, span, q_ref, kv_ref, order_ref, out_ref, qs, k1, v1, k2, v2, raw1, raw2, w1, w2
):
    head_size = k1.shape[1]
    me = lax.axis_index("ctx")
    first = order_ref[2 * me]
    second = order_ref[2 * me + 1]
    p = jnp.minimum(first, second)
    swapped = second < first
    low_at = swapped.astype(jnp.int32)
    pad_high = lax.rem(p, 2)
    pad_low = 1 - pad_high
    chunks_low = (p + 1 + pad_low) // 2
    halves = (slice(0, span), slice(span, 2 * span))

    def rows_of(slot):
        return pl.ds(pl.multiple_of(slot * span, span), span)

    def put(slot, block, half, is_low):
        k2[rows_of(slot), :] = kv_ref[block, 0, rows_of(half), :]
        value = kv_ref[block, 1, rows_of(half), :]
        zero = jnp.zeros_like(value)
        v2[rows_of(slot), :head_size] = jnp.where(is_low, value, zero)
        v2[rows_of(slot), head_size:] = jnp.where(is_low, zero, value)

    put(1, me, low_at, True)
    put(n, me, low_at, False)
    put(0, me, low_at, True)
    put(n + 1, me, 1 - low_at, False)

    def place(d, carry):
        q = jnp.minimum(order_ref[2 * d], order_ref[2 * d + 1])
        lo = (order_ref[2 * d + 1] < order_ref[2 * d]).astype(jnp.int32)
        is_low = q < p

        @pl.when(q != p)
        def _():
            slot = jnp.where(is_low, q + 1 + pad_low, n + 1 - pad_high - (q - p))
            put(slot, d, jnp.where(is_low, lo, 1 - lo), is_low)

        k1[rows_of(d), :] = kv_ref[d, 0, rows_of(lo), :]
        v1[rows_of(d), :head_size] = kv_ref[d, 1, rows_of(lo), :]
        return carry

    lax.fori_loop(0, n, place, 0)
    v1[:, head_size:] = jnp.ones_like(v1[:, head_size:])
    for h in range(heads):
        cols = slice(h * head_size, (h + 1) * head_size)
        pair = [q_ref[s, cols] for s in halves]
        qs[0, h] = jnp.where(swapped, pair[1], pair[0])
        qs[1, h] = jnp.where(swapped, pair[0], pair[1])

    factor = math.log2(math.e) / math.sqrt(head_size)
    ahead = lax.broadcasted_iota(jnp.int32, (span, span), 1) - lax.broadcasted_iota(
        jnp.int32, (span, span), 0
    )
    kept_first = jnp.concatenate([ahead <= 0, ahead <= span - 2 * span * pad_low], axis=1)
    kept_last = jnp.concatenate([ahead <= span - 2 * span * pad_high, ahead <= 0], axis=1)
    chunks1 = n // 2
    chunks2 = n // 2 + 1
    wide = 2 * span

    def scores(q, keys):
        return (
            lax.dot_general(q, keys, (((1,), (1,)), ((), ())), preferred_element_type=jnp.float32)
            * factor
        )

    def folded(x, op):
        return op(x[:, :span], x[:, span:])

    def one_head(h, b):
        high = jnp.full((span, span), NEG, jnp.float32)
        low = high
        for i in range(chunks1):
            cols = slice(i * wide, (i + 1) * wide)
            score = scores(qs[1, h], k1[cols, :])
            raw1[b, :, cols] = score
            high = jnp.maximum(high, folded(score, jnp.maximum))
        for i in range(chunks2):
            cols = slice(i * wide, (i + 1) * wide)
            is_low = i < chunks_low
            score = scores(qs[1 - is_low.astype(jnp.int32), h], k2[cols, :])
            if i == 0:
                score = jnp.where(kept_first, score, NEG)
            if i == chunks2 - 1:
                score = jnp.where(kept_last, score, NEG)
            raw2[b, :, cols] = score
            most = folded(score, jnp.maximum)
            low = jnp.where(is_low, jnp.maximum(low, most), low)
            high = jnp.where(is_low, high, jnp.maximum(high, most))
        low = jnp.broadcast_to(jnp.max(low, axis=1, keepdims=True), (span, span))
        high = jnp.broadcast_to(jnp.max(high, axis=1, keepdims=True), (span, span))
        for i in range(chunks1):
            cols = slice(i * wide, (i + 1) * wide)
            shift = jnp.concatenate([high, high], axis=1)
            w1[b, :, cols] = jnp.exp2(raw1[b, :, cols] - shift).astype(jnp.bfloat16)
        sum_low = jnp.zeros((span, span), jnp.float32)
        sum_high = sum_low
        for i in range(chunks2):
            cols = slice(i * wide, (i + 1) * wide)
            is_low = i < chunks_low
            shift = jnp.where(is_low, low, high)
            weight = jnp.exp2(raw2[b, :, cols] - jnp.concatenate([shift, shift], axis=1))
            w2[b, :, cols] = weight.astype(jnp.bfloat16)
            add = folded(weight, jnp.add)
            sum_low = jnp.where(is_low, sum_low + add, sum_low)
            sum_high = jnp.where(is_low, sum_high, sum_high + add)
        got1 = jnp.dot(w1[b], v1[...], preferred_element_type=jnp.float32)
        got2 = jnp.dot(w2[b], v2[...], preferred_element_type=jnp.float32)
        sum_low = jnp.sum(sum_low, axis=1, keepdims=True)
        sum_high = jnp.sum(sum_high, axis=1, keepdims=True)
        out_low = got2[:, :head_size] / sum_low
        out_high = (got1[:, :head_size] + got2[:, head_size:]) / (got1[:, head_size:] + sum_high)
        cols = pl.ds(pl.multiple_of(h * head_size, head_size), head_size)
        out_ref[halves[0], cols] = jnp.where(swapped, out_high, out_low).astype(jnp.bfloat16)
        out_ref[halves[1], cols] = jnp.where(swapped, out_low, out_high).astype(jnp.bfloat16)

    together = 2 if chunks1 <= heads else 1

    def some_heads(g, carry):
        for b in range(together):
            one_head(g * together + b, b)
        return carry

    lax.fori_loop(0, heads // together, some_heads, 0)


LOW, HIGH = 0, 1
EXTRA = 16


def fused_kernel(
    n, heads, span, order_ref, q_hbm, k_hbm, v_hbm, out_ref,
    buf, q_in, qt, acc, top, raw, part, wide_v, load_sem, send_sem, recv_sem,
):
    lanes = 4
    zs = n // lanes
    head_size = buf.shape[3]
    rows = heads * span
    tile = 2 * span
    tiles = rows // tile
    tall = head_size + EXTRA
    me = lax.axis_index("ctx")
    z = me // lanes
    lane = lax.rem(me, lanes)
    y = lane // 2
    c = lax.rem(lane, 2)
    side = z * lanes + (1 - y) * 2 + c
    twin = z * lanes + y * 2 + (1 - c)
    not_top = z < zs - 1
    not_bottom = z > 0
    up = jnp.minimum(me + lanes, n - lanes + lane)
    down = jnp.maximum(me - lanes, lane)
    target = (up, down, side, twin)

    load_k = pltpu.make_async_copy(k_hbm, buf.at[me, 0], load_sem.at[0])
    load_v = pltpu.make_async_copy(v_hbm, buf.at[me, 1], load_sem.at[1])
    load_q = pltpu.make_async_copy(q_hbm, q_in, load_sem.at[2])
    load_k.start()
    load_v.start()
    load_q.start()

    barrier = pltpu.get_barrier_semaphore()

    def greet(who):
        pl.semaphore_signal(
            barrier, inc=1, device_id={"ctx": who}, device_id_type=pl.DeviceIdType.MESH
        )

    greet(side)
    greet(twin)
    pl.when(not_top)(lambda: greet(up))
    pl.when(not_bottom)(lambda: greet(down))
    load_k.wait()
    load_v.wait()
    pl.semaphore_wait(barrier, 2 + not_top.astype(jnp.int32) + not_bottom.astype(jnp.int32))

    def copy(block, kv, route):
        return pltpu.make_async_remote_copy(
            src_ref=buf.at[block, kv],
            dst_ref=buf.at[block, kv],
            send_sem=send_sem.at[block, kv, route],
            recv_sem=recv_sem.at[block, kv],
            device_id={"ctx": target[route]},
            device_id_type=pl.DeviceIdType.MESH,
        )

    for kv in range(2):
        pl.when(not_top)(lambda: copy(me, kv, UP).start())
        pl.when(not_bottom)(lambda: copy(me, kv, DOWN).start())
        copy(me, kv, SIDE).start()
        copy(me, kv, TWIN).start()

    def at(zz, yy, cc):
        return zz * lanes + yy * 2 + cc

    def from_line(zz, onward, keep):
        block = at(zz, y, c)
        for kv in range(2):
            copy(block, kv, onward).wait_recv()
            pl.when(keep)(lambda: copy(block, kv, onward).start())
            copy(block, kv, SIDE).start()
            copy(block, kv, TWIN).start()

    def from_side(zz):
        block = at(zz, 1 - y, c)
        for kv in range(2):
            copy(block, kv, TWIN).wait_recv()
            copy(block, kv, TWIN).start()

    def from_twin(zz, yy):
        for kv in range(2):
            copy(at(zz, yy, 1 - c), kv, TWIN).wait_recv()

    def both(s, low, high):
        pl.when(z >= s)(lambda: low(z - s))
        pl.when(z + s < zs)(lambda: high(z + s))

    def lines(s):
        both(s, lambda zz: from_line(zz, UP, not_top), lambda zz: from_line(zz, DOWN, not_bottom))

    def sides(s):
        if s == 0:
            from_side(z)
        else:
            both(s, from_side, from_side)

    inner = jnp.minimum(z, zs - 1 - z)
    outward = jnp.where(z < zs - 1 - z, 1, -1)

    def plane(r):
        near = z + ((r + 1) // 2) * (1 if r % 2 == 0 else -1)
        return jnp.where(r <= 2 * inner, near, z + (r - inner) * outward)

    def pair_of(d):
        first = order_ref[2 * d]
        second = order_ref[2 * d + 1]
        return jnp.minimum(first, second), second < first

    p, swapped = pair_of(me)
    factor = math.log2(math.e) / math.sqrt(head_size)
    spans = (slice(0, span), slice(span, 2 * span))

    load_q.wait()
    for h in range(heads):
        cols = slice(h * head_size, (h + 1) * head_size)
        dest = slice(h * span, (h + 1) * span)
        a = q_in[spans[0], cols]
        b = q_in[spans[1], cols]
        qt[LOW, :, dest] = jnp.where(swapped, b, a).T
        qt[HIGH, :, dest] = jnp.where(swapped, a, b).T

    def lane_tile(t):
        return slice(t * tile, (t + 1) * tile)

    def peak(score):
        return jnp.max(score.reshape(span // 8, 8, tile), axis=0)

    def spread(m):
        return jnp.broadcast_to(jnp.max(m, axis=0, keepdims=True), (8, tile))

    def weigh(slot, m):
        score = raw[slot].reshape(span // 8, 8, tile)
        return jnp.exp2(score - m[None]).reshape(span, tile).astype(jnp.bfloat16)

    def scores(keys, which, t):
        return (
            jnp.dot(keys, qt[which, :, lane_tile(t)], preferred_element_type=jnp.float32) * factor
        )

    def halves_of(d, kv, flip):
        a = buf[d, kv, spans[0], :]
        b = buf[d, kv, spans[1], :]
        return jnp.where(flip, b, a), jnp.where(flip, a, b)

    ones = jnp.ones((EXTRA, span), jnp.bfloat16)
    wide_v[head_size:tall, :] = jnp.ones_like(wide_v[head_size:tall, :])

    def own():
        k_low, k_high = halves_of(me, 0, swapped)
        v_low, v_high = halves_of(me, 1, swapped)
        wide_v[:head_size, :span] = v_low.T
        wide_v[:head_size, span : 2 * span] = v_high.T
        kept = lax.broadcasted_iota(jnp.int32, (span, tile), 0) <= lax.rem(
            lax.broadcasted_iota(jnp.int32, (span, tile), 1), span
        )
        for t in range(tiles):
            lt = lane_tile(t)
            s0 = scores(k_low, HIGH, t)
            s1 = jnp.where(kept, scores(k_high, HIGH, t), NEG)
            s2 = jnp.where(kept, scores(k_low, LOW, t), NEG)
            raw[0], raw[1], raw[2] = s0, s1, s2
            m_high = spread(jnp.maximum(peak(s0), peak(s1)))
            m_low = spread(peak(s2))
            top[HIGH, :, lt] = m_high
            top[LOW, :, lt] = m_low
            part[0, :span, :] = weigh(0, m_high)
            part[0, span : 2 * span, :] = weigh(1, m_high)
            part[1, :span, :] = weigh(2, m_low)
            acc[HIGH, :, lt] = jnp.dot(
                wide_v[:tall, : 2 * span], part[0, : 2 * span, :], preferred_element_type=jnp.float32
            )
            acc[LOW, :, lt] = jnp.dot(
                wide_v[:tall, :span], part[1, :span, :], preferred_element_type=jnp.float32
            )

    def group(blocks, between=()):
        g = len(blocks)
        depth = g * span
        info = []
        for j, d in enumerate(blocks):
            q, flip = pair_of(d)
            is_low = q < p
            k_low, k_high = halves_of(d, 0, flip)
            v_low, v_high = halves_of(d, 1, flip)
            at_j = slice(j * span, (j + 1) * span)
            wide_v[:head_size, at_j] = v_low.T
            v_x = jnp.where(is_low, v_low, v_high).T
            nil = jnp.zeros_like(v_x)
            wide_v[tall : tall + head_size, at_j] = jnp.where(is_low, v_x, nil)
            wide_v[tall + head_size : 2 * tall, at_j] = jnp.where(is_low, ones, jnp.zeros_like(ones))
            wide_v[2 * tall : 2 * tall + head_size, at_j] = jnp.where(is_low, nil, v_x)
            wide_v[2 * tall + head_size :, at_j] = jnp.where(is_low, jnp.zeros_like(ones), ones)
            info.append((is_low, k_low, jnp.where(is_low, k_low, k_high)))
        for t in range(tiles):
            lt = lane_tile(t)
            old_high = top[HIGH, :, lt]
            old_low = top[LOW, :, lt]
            high, low = old_high, old_low
            base = (t % 2) * 8
            for j, (is_low, k_low, k_x) in enumerate(info):
                s = scores(k_low, HIGH, t)
                raw[base + 2 * j] = s
                high = jnp.maximum(high, peak(s))
                s = scores(k_x, 1 - is_low.astype(jnp.int32), t)
                raw[base + 2 * j + 1] = s
                m = peak(s)
                low = jnp.where(is_low, jnp.maximum(low, m), low)
                high = jnp.where(is_low, high, jnp.maximum(high, m))
            high = spread(high)
            low = spread(low)
            top[HIGH, :, lt] = high
            top[LOW, :, lt] = low
            pb = (t % 2) * 2
            for j, (is_low, _, _) in enumerate(info):
                at_j = slice(j * span, (j + 1) * span)
                part[pb, at_j, :] = weigh(base + 2 * j, high)
                part[pb + 1, at_j, :] = weigh(base + 2 * j + 1, jnp.where(is_low, low, high))
            more = jnp.dot(
                wide_v[:tall, :depth], part[pb, :depth, :], preferred_element_type=jnp.float32
            )
            mixed = jnp.dot(
                wide_v[tall:, :depth], part[pb + 1, :depth, :], preferred_element_type=jnp.float32
            )

            def scaled(which, old, new):
                return (
                    acc[which, :, lt].reshape(tall // 8, 8, tile) * jnp.exp2(old - new)[None]
                ).reshape(tall, tile)

            acc[HIGH, :, lt] = scaled(HIGH, old_high, high) + (more + mixed[tall:])
            acc[LOW, :, lt] = scaled(LOW, old_low, low) + mixed[:tall]
            if t < len(between):
                between[t]()

    own()
    lines(1)
    sides(0)
    from_twin(z, y)
    from_twin(z, 1 - y)
    group([twin, side, at(z, 1 - y, 1 - c)])
    for r in range(1, zs):
        if r + 1 < zs:
            lines(r + 1)
        sides(r)
        zz = plane(r)
        if r + 1 == zs:
            from_twin(zz, y)
            group([at(zz, y, c), at(zz, y, 1 - c)])
            from_twin(zz, 1 - y)
            group([at(zz, 1 - y, c), at(zz, 1 - y, 1 - c)])
        else:
            from_twin(zz, y)
            from_twin(zz, 1 - y)
            group([at(zz, y, c), at(zz, y, 1 - c), at(zz, 1 - y, c), at(zz, 1 - y, 1 - c)])

    for h in range(heads):
        cols = slice(h * head_size, (h + 1) * head_size)
        src = slice(h * span, (h + 1) * span)
        outs = []
        for which in (LOW, HIGH):
            total = acc[which, head_size : head_size + 8, src]
            share = acc[which, :head_size, src].reshape(head_size // 8, 8, span) / total[None]
            outs.append(share.reshape(head_size, span).astype(jnp.bfloat16).T)
        out_ref[spans[0], cols] = jnp.where(swapped, outs[HIGH], outs[LOW])
        out_ref[spans[1], cols] = jnp.where(swapped, outs[LOW], outs[HIGH])

    for kv in range(2):
        pl.when(not_top)(lambda: copy(me, kv, UP).wait_send())
        pl.when(not_bottom)(lambda: copy(me, kv, DOWN).wait_send())
        copy(me, kv, SIDE).wait_send()
        copy(me, kv, TWIN).wait_send()

    def line_sent(zz, onward, keep):
        for kv in range(2):
            pl.when(keep)(lambda: copy(at(zz, y, c), kv, onward).wait_send())
            copy(at(zz, y, c), kv, SIDE).wait_send()
            copy(at(zz, y, c), kv, TWIN).wait_send()

    def side_sent(zz):
        for kv in range(2):
            copy(at(zz, 1 - y, c), kv, TWIN).wait_send()

    side_sent(z)
    for s in range(1, zs):
        both(s, lambda zz: line_sent(zz, UP, not_top), lambda zz: line_sent(zz, DOWN, not_bottom))
        both(s, side_sent, side_sent)


def fused(n, queries, keys, values, span_order):
    local_rows, width = queries.shape
    head_size = keys.shape[1]
    heads = width // head_size
    span = local_rows // 2
    rows = heads * span
    anywhere = pl.BlockSpec(memory_space=pl.ANY)
    tall = head_size + EXTRA
    return pl.pallas_call(
        functools.partial(fused_kernel, n, heads, span),
        out_shape=jax.ShapeDtypeStruct((local_rows, width), jnp.bfloat16),
        in_specs=[pl.BlockSpec(memory_space=pltpu.SMEM), anywhere, anywhere, anywhere],
        out_specs=pl.BlockSpec(memory_space=pltpu.VMEM),
        scratch_shapes=[
            pltpu.VMEM((n, 2, local_rows, head_size), jnp.bfloat16),
            pltpu.VMEM((local_rows, width), jnp.bfloat16),
            pltpu.VMEM((2, head_size, rows), jnp.bfloat16),
            pltpu.VMEM((2, tall, rows), jnp.float32),
            pltpu.VMEM((2, 8, rows), jnp.float32),
            pltpu.VMEM((16, span, 2 * span), jnp.float32),
            pltpu.VMEM((4, 4 * span, 2 * span), jnp.bfloat16),
            pltpu.VMEM((3 * tall, 4 * span), jnp.bfloat16),
            pltpu.SemaphoreType.DMA((3,)),
            pltpu.SemaphoreType.DMA((n, 2, 4)),
            pltpu.SemaphoreType.DMA((n, 2)),
        ],
        compiler_params=pltpu.CompilerParams(collective_id=0, has_side_effects=True),
        name="fused",
    )(span_order, queries, keys, values)


def body(n, queries, keys, values, span_order):
    if n <= FUSED_MOST:
        return fused(n, queries, keys, values, span_order)
    local_rows, width = queries.shape
    head_size = keys.shape[1]
    heads = width // head_size
    span = local_rows // 2
    vmem = pl.BlockSpec(memory_space=pltpu.VMEM)
    gathered = pl.pallas_call(
        functools.partial(gather_kernel, n),
        out_shape=jax.ShapeDtypeStruct((n, 2, local_rows, head_size), jnp.bfloat16),
        in_specs=[vmem, vmem],
        out_specs=vmem,
        scratch_shapes=[
            pltpu.SemaphoreType.DMA((n, 2, 4)),
            pltpu.SemaphoreType.DMA((n, 2)),
        ],
        compiler_params=pltpu.CompilerParams(collective_id=0, has_side_effects=True),
        name="gather",
    )(keys, values)
    half_keys = n * span
    more_keys = (n + 2) * span
    return pl.pallas_call(
        functools.partial(attend_kernel, n, heads, span),
        out_shape=jax.ShapeDtypeStruct((local_rows, width), jnp.bfloat16),
        in_specs=[vmem, vmem, pl.BlockSpec(memory_space=pltpu.SMEM)],
        out_specs=vmem,
        scratch_shapes=[
            pltpu.VMEM((2, heads, span, head_size), jnp.bfloat16),
            pltpu.VMEM((half_keys, head_size), jnp.bfloat16),
            pltpu.VMEM((half_keys, 2 * head_size), jnp.bfloat16),
            pltpu.VMEM((more_keys, head_size), jnp.bfloat16),
            pltpu.VMEM((more_keys, 2 * head_size), jnp.bfloat16),
            pltpu.VMEM((2, span, half_keys), jnp.float32),
            pltpu.VMEM((2, span, more_keys), jnp.float32),
            pltpu.VMEM((2, span, half_keys), jnp.bfloat16),
            pltpu.VMEM((2, span, more_keys), jnp.bfloat16),
        ],
        name="attend",
    )(queries, gathered, span_order)


def solution(mesh):
    in_specs = (
        P(("groups", "ctx"), None),
        P(("groups", "ctx"), None),
        P(("groups", "ctx"), None),
        P("groups"),
    )
    out_specs = P(("groups", "ctx"), None)
    return jax.shard_map(
        functools.partial(body, mesh.shape["ctx"]),
        mesh=mesh,
        in_specs=in_specs,
        out_specs=out_specs,
        check_vma=False,
    )
```

```python
import functools
import math

import jax
import jax.numpy as jnp
from jax import lax
from jax.experimental import pallas as pl
from jax.experimental.pallas import tpu as pltpu
from jax.sharding import PartitionSpec as P

UP, DOWN, SIDE, TWIN = 0, 1, 2, 3
NEG = -1e30
FUSED_MOST = 32
PIECES = 2
RELIEF = True
GRANT = 24 << 20


def gather_kernel(n, k_ref, v_ref, buf, send_sem, recv_sem):
    lanes = 4
    zs = n // lanes
    me = lax.axis_index("ctx")
    z = me // lanes
    lane = lax.rem(me, lanes)
    y = lane // 2
    c = lax.rem(lane, 2)
    side = z * lanes + (1 - y) * 2 + c
    twin = z * lanes + y * 2 + (1 - c)
    not_top = z < zs - 1
    not_bottom = z > 0
    up = jnp.minimum(me + lanes, n - lanes + lane)
    down = jnp.maximum(me - lanes, lane)
    target = (up, down, side, twin)

    barrier = pltpu.get_barrier_semaphore()

    def greet(who):
        pl.semaphore_signal(
            barrier, inc=1, device_id={"ctx": who}, device_id_type=pl.DeviceIdType.MESH
        )

    greet(side)
    greet(twin)
    pl.when(not_top)(lambda: greet(up))
    pl.when(not_bottom)(lambda: greet(down))
    pl.semaphore_wait(barrier, 2 + not_top.astype(jnp.int32) + not_bottom.astype(jnp.int32))

    def copy(block, kv, route, src=None):
        return pltpu.make_async_remote_copy(
            src_ref=buf.at[block, kv] if src is None else src,
            dst_ref=buf.at[block, kv],
            send_sem=send_sem.at[block, kv, route],
            recv_sem=recv_sem.at[block, kv],
            device_id={"ctx": target[route]},
            device_id_type=pl.DeviceIdType.MESH,
        )

    own = (k_ref, v_ref)
    for kv in range(2):
        pl.when(not_top)(lambda: copy(me, kv, UP, own[kv]).start())
        pl.when(not_bottom)(lambda: copy(me, kv, DOWN, own[kv]).start())
        copy(me, kv, SIDE, own[kv]).start()
        copy(me, kv, TWIN, own[kv]).start()
    buf[me, 0] = k_ref[...]
    buf[me, 1] = v_ref[...]

    def at(zz, yy, cc):
        return zz * lanes + yy * 2 + cc

    def from_line(zz, onward, keep):
        block = at(zz, y, c)
        for kv in range(2):
            copy(block, kv, onward).wait_recv()
            pl.when(keep)(lambda: copy(block, kv, onward).start())
            copy(block, kv, SIDE).start()
            copy(block, kv, TWIN).start()

    def from_side(zz):
        block = at(zz, 1 - y, c)
        for kv in range(2):
            copy(block, kv, TWIN).wait_recv()
            copy(block, kv, TWIN).start()

    def from_twin(zz):
        for yy in (y, 1 - y):
            for kv in range(2):
                copy(at(zz, yy, 1 - c), kv, TWIN).wait_recv()

    def both(s, low, high):
        pl.when(z >= s)(lambda: low(z - s))
        pl.when(z + s < zs)(lambda: high(z + s))

    for s in range(1, zs):
        both(s, lambda zz: from_line(zz, UP, not_top), lambda zz: from_line(zz, DOWN, not_bottom))
        if s == 1:
            from_side(z)
        else:
            both(s - 1, from_side, from_side)
    both(zs - 1, from_side, from_side)
    from_twin(z)
    for s in range(1, zs):
        both(s, from_twin, from_twin)

    for kv in range(2):
        pl.when(not_top)(lambda: copy(me, kv, UP, own[kv]).wait_send())
        pl.when(not_bottom)(lambda: copy(me, kv, DOWN, own[kv]).wait_send())
        copy(me, kv, SIDE, own[kv]).wait_send()
        copy(me, kv, TWIN, own[kv]).wait_send()

    def line_sent(zz, onward, keep):
        for kv in range(2):
            pl.when(keep)(lambda: copy(at(zz, y, c), kv, onward).wait_send())
            copy(at(zz, y, c), kv, SIDE).wait_send()
            copy(at(zz, y, c), kv, TWIN).wait_send()

    def side_sent(zz):
        for kv in range(2):
            copy(at(zz, 1 - y, c), kv, TWIN).wait_send()

    side_sent(z)
    for s in range(1, zs):
        both(s, lambda zz: line_sent(zz, UP, not_top), lambda zz: line_sent(zz, DOWN, not_bottom))
        both(s, side_sent, side_sent)


def attend_kernel(
    n, heads, span, q_ref, kv_ref, order_ref, out_ref, qs, k1, v1, k2, v2, raw1, raw2, w1, w2
):
    head_size = k1.shape[1]
    me = lax.axis_index("ctx")
    first = order_ref[2 * me]
    second = order_ref[2 * me + 1]
    p = jnp.minimum(first, second)
    swapped = second < first
    low_at = swapped.astype(jnp.int32)
    pad_high = lax.rem(p, 2)
    pad_low = 1 - pad_high
    chunks_low = (p + 1 + pad_low) // 2
    halves = (slice(0, span), slice(span, 2 * span))

    def rows_of(slot):
        return pl.ds(pl.multiple_of(slot * span, span), span)

    def put(slot, block, half, is_low):
        k2[rows_of(slot), :] = kv_ref[block, 0, rows_of(half), :]
        value = kv_ref[block, 1, rows_of(half), :]
        zero = jnp.zeros_like(value)
        v2[rows_of(slot), :head_size] = jnp.where(is_low, value, zero)
        v2[rows_of(slot), head_size:] = jnp.where(is_low, zero, value)

    put(1, me, low_at, True)
    put(n, me, low_at, False)
    put(0, me, low_at, True)
    put(n + 1, me, 1 - low_at, False)

    def place(d, carry):
        q = jnp.minimum(order_ref[2 * d], order_ref[2 * d + 1])
        lo = (order_ref[2 * d + 1] < order_ref[2 * d]).astype(jnp.int32)
        is_low = q < p

        @pl.when(q != p)
        def _():
            slot = jnp.where(is_low, q + 1 + pad_low, n + 1 - pad_high - (q - p))
            put(slot, d, jnp.where(is_low, lo, 1 - lo), is_low)

        k1[rows_of(d), :] = kv_ref[d, 0, rows_of(lo), :]
        v1[rows_of(d), :head_size] = kv_ref[d, 1, rows_of(lo), :]
        return carry

    lax.fori_loop(0, n, place, 0)
    v1[:, head_size:] = jnp.ones_like(v1[:, head_size:])
    for h in range(heads):
        cols = slice(h * head_size, (h + 1) * head_size)
        pair = [q_ref[s, cols] for s in halves]
        qs[0, h] = jnp.where(swapped, pair[1], pair[0])
        qs[1, h] = jnp.where(swapped, pair[0], pair[1])

    factor = math.log2(math.e) / math.sqrt(head_size)
    ahead = lax.broadcasted_iota(jnp.int32, (span, span), 1) - lax.broadcasted_iota(
        jnp.int32, (span, span), 0
    )
    kept_first = jnp.concatenate([ahead <= 0, ahead <= span - 2 * span * pad_low], axis=1)
    kept_last = jnp.concatenate([ahead <= span - 2 * span * pad_high, ahead <= 0], axis=1)
    chunks1 = n // 2
    chunks2 = n // 2 + 1
    wide = 2 * span

    def scores(q, keys):
        return (
            lax.dot_general(q, keys, (((1,), (1,)), ((), ())), preferred_element_type=jnp.float32)
            * factor
        )

    def folded(x, op):
        return op(x[:, :span], x[:, span:])

    def one_head(h, b):
        high = jnp.full((span, span), NEG, jnp.float32)
        low = high
        for i in range(chunks1):
            cols = slice(i * wide, (i + 1) * wide)
            score = scores(qs[1, h], k1[cols, :])
            raw1[b, :, cols] = score
            high = jnp.maximum(high, folded(score, jnp.maximum))
        for i in range(chunks2):
            cols = slice(i * wide, (i + 1) * wide)
            is_low = i < chunks_low
            score = scores(qs[1 - is_low.astype(jnp.int32), h], k2[cols, :])
            if i == 0:
                score = jnp.where(kept_first, score, NEG)
            if i == chunks2 - 1:
                score = jnp.where(kept_last, score, NEG)
            raw2[b, :, cols] = score
            most = folded(score, jnp.maximum)
            low = jnp.where(is_low, jnp.maximum(low, most), low)
            high = jnp.where(is_low, high, jnp.maximum(high, most))
        low = jnp.broadcast_to(jnp.max(low, axis=1, keepdims=True), (span, span))
        high = jnp.broadcast_to(jnp.max(high, axis=1, keepdims=True), (span, span))
        for i in range(chunks1):
            cols = slice(i * wide, (i + 1) * wide)
            shift = jnp.concatenate([high, high], axis=1)
            w1[b, :, cols] = jnp.exp2(raw1[b, :, cols] - shift).astype(jnp.bfloat16)
        sum_low = jnp.zeros((span, span), jnp.float32)
        sum_high = sum_low
        for i in range(chunks2):
            cols = slice(i * wide, (i + 1) * wide)
            is_low = i < chunks_low
            shift = jnp.where(is_low, low, high)
            weight = jnp.exp2(raw2[b, :, cols] - jnp.concatenate([shift, shift], axis=1))
            w2[b, :, cols] = weight.astype(jnp.bfloat16)
            add = folded(weight, jnp.add)
            sum_low = jnp.where(is_low, sum_low + add, sum_low)
            sum_high = jnp.where(is_low, sum_high, sum_high + add)
        got1 = jnp.dot(w1[b], v1[...], preferred_element_type=jnp.float32)
        got2 = jnp.dot(w2[b], v2[...], preferred_element_type=jnp.float32)
        sum_low = jnp.sum(sum_low, axis=1, keepdims=True)
        sum_high = jnp.sum(sum_high, axis=1, keepdims=True)
        out_low = got2[:, :head_size] / sum_low
        out_high = (got1[:, :head_size] + got2[:, head_size:]) / (got1[:, head_size:] + sum_high)
        cols = pl.ds(pl.multiple_of(h * head_size, head_size), head_size)
        out_ref[halves[0], cols] = jnp.where(swapped, out_high, out_low).astype(jnp.bfloat16)
        out_ref[halves[1], cols] = jnp.where(swapped, out_low, out_high).astype(jnp.bfloat16)

    together = 2 if chunks1 <= heads else 1

    def some_heads(g, carry):
        for b in range(together):
            one_head(g * together + b, b)
        return carry

    lax.fori_loop(0, heads // together, some_heads, 0)


LOW, HIGH = 0, 1
EXTRA = 16


def fused_kernel(
    n, heads, span, order_hbm, q_hbm, k_hbm, v_hbm, acc,
    order_ref, buf, q_in, qt, top, raw, part, wide_v, load_sem, send_sem, line_sem, side_sem, twin_sem,
):
    lanes = 4
    zs = n // lanes
    head_size = buf.shape[3]
    rows = heads * span
    tile = 2 * span
    tiles = rows // tile
    tall = head_size + EXTRA
    me = lax.axis_index("ctx")
    z = me // lanes
    lane = lax.rem(me, lanes)
    y = lane // 2
    c = lax.rem(lane, 2)
    side = z * lanes + (1 - y) * 2 + c
    twin = z * lanes + y * 2 + (1 - c)
    not_top = z < zs - 1
    not_bottom = z > 0
    up = jnp.minimum(me + lanes, n - lanes + lane)
    down = jnp.maximum(me - lanes, lane)
    target = (up, down, side, twin)

    load_k = pltpu.make_async_copy(k_hbm, buf.at[me, 0], load_sem.at[0])
    load_v = pltpu.make_async_copy(v_hbm, buf.at[me, 1], load_sem.at[1])
    load_q = pltpu.make_async_copy(q_hbm, q_in, load_sem.at[2])
    load_order = pltpu.make_async_copy(order_hbm, order_ref, load_sem.at[3])
    load_k.start()
    load_v.start()
    load_order.start()
    load_q.start()

    barrier = pltpu.get_barrier_semaphore()

    def greet(who):
        pl.semaphore_signal(
            barrier, inc=1, device_id={"ctx": who}, device_id_type=pl.DeviceIdType.MESH
        )

    greet(side)
    greet(twin)
    pl.when(not_top)(lambda: greet(up))
    pl.when(not_bottom)(lambda: greet(down))
    load_k.wait()
    load_v.wait()
    pl.semaphore_wait(barrier, 2 + not_top.astype(jnp.int32) + not_bottom.astype(jnp.int32))

    piece = span * 2 // PIECES

    def copy(zz, yy, kv, part_of, route):
        block = at(zz, yy, c)
        where = buf.at[block, kv, pl.ds(part_of * piece, piece)]
        other = yy is not y
        if route == SIDE:
            landed = side_sem.at[zz, kv, part_of]
        elif route == TWIN:
            landed = twin_sem.at[zz, int(other)]
        elif other:
            landed = side_sem.at[zz, kv, part_of]
        else:
            landed = line_sem.at[zz, kv, part_of]
        return pltpu.make_async_remote_copy(
            src_ref=where,
            dst_ref=where,
            send_sem=send_sem.at[route],
            recv_sem=landed,
            device_id={"ctx": target[route]},
            device_id_type=pl.DeviceIdType.MESH,
        )

    def at(zz, yy, cc):
        return zz * lanes + yy * 2 + cc

    far_y = 1 - y
    at_bottom = z == 0
    at_top = z == zs - 1

    def early(zz, kv):
        if kv == 0 or zs <= 2 or not RELIEF:
            return jnp.bool_(False)
        return jnp.logical_or(zz == 0, zz == zs - 1)

    def sends_own(act):
        for kv in range(2):
            for i in range(PIECES):
                pl.when(not_top)(lambda: act(copy(z, y, kv, i, UP)))
                pl.when(not_bottom)(lambda: act(copy(z, y, kv, i, DOWN)))
                act(copy(z, y, kv, i, SIDE))
                act(copy(z, y, kv, i, TWIN))

    def sends_line(zz, kv, i, onward, act):
        pl.when(not_top if onward == UP else not_bottom)(lambda: act(copy(zz, y, kv, i, onward)))
        pl.when(jnp.logical_not(early(zz, kv)))(lambda: act(copy(zz, y, kv, i, SIDE)))
        act(copy(zz, y, kv, i, TWIN))

    def sends_side(zz, kv, i, onward, act):
        more = not_top if onward == UP else not_bottom
        if kv == 1 and zs > 2 and RELIEF:
            pl.when(jnp.logical_and(early(zz, kv), more))(lambda: act(copy(zz, far_y, kv, i, onward)))
        act(copy(zz, far_y, kv, i, TWIN))

    def sends_near(kv, i, act):
        if kv == 1 and zs > 2 and RELIEF:
            pl.when(at_bottom)(lambda: act(copy(z, far_y, kv, i, UP)))
            pl.when(at_top)(lambda: act(copy(z, far_y, kv, i, DOWN)))
        act(copy(z, far_y, kv, i, TWIN))

    def begin(one):
        one.start()

    def arrived(zz, yy, kv, i):
        where = buf.at[at(zz, yy, c), kv, pl.ds(i * piece, piece)]
        sem = (line_sem if yy is y else side_sem).at[zz, kv, i]
        pltpu.make_async_copy(where, where, sem).wait()

    def both(s, low, high):
        pl.when(z >= s)(lambda: low(z - s))
        pl.when(z + s < zs)(lambda: high(z + s))

    def line_event(s, kv, i):
        def arrive(zz, onward):
            arrived(zz, y, kv, i)
            sends_line(zz, kv, i, onward, begin)

        both(s, lambda zz: arrive(zz, UP), lambda zz: arrive(zz, DOWN))

    def side_event(s, kv, i):
        def arrive(zz, onward):
            arrived(zz, far_y, kv, i)
            sends_side(zz, kv, i, onward, begin)

        if s:
            both(s, lambda zz: arrive(zz, UP), lambda zz: arrive(zz, DOWN))
        else:
            arrived(z, far_y, kv, i)
            sends_near(kv, i, begin)

    def events(kind, s):
        return [functools.partial(kind, s, kv, i) for kv in range(2) for i in range(PIECES)]

    def from_twin(zz, yy):
        where = buf.at[at(zz, yy, 1 - c)]
        pltpu.make_async_copy(where, where, twin_sem.at[zz, int(yy is not y)]).wait()

    def all_sent():
        def taken(arrays, route):
            blocks = arrays // 2
            where = buf.at[pl.ds(0, blocks)] if blocks else buf.at[0, 0]
            pltpu.make_async_copy(where, where, send_sem.at[route]).wait()

        taken(4 * zs, TWIN)
        if not RELIEF or zs <= 2:
            taken(2 * zs, SIDE)
            for zz in range(zs):
                pl.when(jnp.logical_and(not_top, zz <= z))(lambda: taken(2, UP))
                pl.when(jnp.logical_and(not_bottom, zz >= z))(lambda: taken(2, DOWN))
        else:
            taken(2, SIDE)
            for zz in range(zs):
                pl.when(zz != z)(lambda: taken(1, SIDE))
                if 0 < zz < zs - 1:
                    pl.when(zz != z)(lambda: taken(1, SIDE))
                pl.when(jnp.logical_and(not_top, zz <= z))(lambda: taken(2, UP))
                pl.when(jnp.logical_and(not_bottom, zz >= z))(lambda: taken(2, DOWN))
            pl.when(not_top)(lambda: taken(1, UP))
            pl.when(not_bottom)(lambda: taken(1, DOWN))

    sends_own(begin)

    inner = jnp.minimum(z, zs - 1 - z)
    outward = jnp.where(z < zs - 1 - z, 1, -1)

    def plane(r):
        near = z + ((r + 1) // 2) * (1 if r % 2 == 0 else -1)
        return jnp.where(r <= 2 * inner, near, z + (r - inner) * outward)

    def pair_of(d):
        first = order_ref[2 * d]
        second = order_ref[2 * d + 1]
        return jnp.minimum(first, second), second < first

    load_order.wait()
    p, swapped = pair_of(me)
    factor = math.log2(math.e) / math.sqrt(head_size)
    spans = (slice(0, span), slice(span, 2 * span))

    load_q.wait()
    for h in range(heads):
        cols = slice(h * head_size, (h + 1) * head_size)
        dest = slice(h * span, (h + 1) * span)
        a = q_in[spans[0], cols]
        b = q_in[spans[1], cols]
        qt[LOW, :, dest] = jnp.where(swapped, b, a).T
        qt[HIGH, :, dest] = jnp.where(swapped, a, b).T

    def lane_tile(t):
        return slice(t * tile, (t + 1) * tile)

    def peak(score):
        return jnp.max(score.reshape(span // 8, 8, tile), axis=0)

    def spread(m):
        return jnp.broadcast_to(jnp.max(m, axis=0, keepdims=True), (8, tile))

    def weigh(slot, m):
        score = raw[slot].reshape(span // 8, 8, tile)
        return jnp.exp2(score - m[None]).reshape(span, tile).astype(jnp.bfloat16)

    def scores(keys, which, t):
        return (
            jnp.dot(keys, qt[which, :, lane_tile(t)], preferred_element_type=jnp.float32) * factor
        )

    def halves_of(d, kv, flip):
        a = buf[d, kv, spans[0], :]
        b = buf[d, kv, spans[1], :]
        return jnp.where(flip, b, a), jnp.where(flip, a, b)

    ones = jnp.ones((EXTRA, span), jnp.bfloat16)
    wide_v[head_size:tall, :] = jnp.ones_like(wide_v[head_size:tall, :])

    def own():
        k_low, k_high = halves_of(me, 0, swapped)
        v_low, v_high = halves_of(me, 1, swapped)
        wide_v[:head_size, :span] = v_low.T
        wide_v[:head_size, span : 2 * span] = v_high.T
        kept = lax.broadcasted_iota(jnp.int32, (span, tile), 0) <= lax.rem(
            lax.broadcasted_iota(jnp.int32, (span, tile), 1), span
        )
        for t in range(tiles):
            lt = lane_tile(t)
            s0 = scores(k_low, HIGH, t)
            s1 = jnp.where(kept, scores(k_high, HIGH, t), NEG)
            s2 = jnp.where(kept, scores(k_low, LOW, t), NEG)
            raw[0], raw[1], raw[2] = s0, s1, s2
            m_high = spread(jnp.maximum(peak(s0), peak(s1)))
            m_low = spread(peak(s2))
            top[HIGH, :, lt] = m_high
            top[LOW, :, lt] = m_low
            part[0, :span, :] = weigh(0, m_high)
            part[0, span : 2 * span, :] = weigh(1, m_high)
            part[1, :span, :] = weigh(2, m_low)
            acc[HIGH, :, lt] = jnp.dot(
                wide_v[:tall, : 2 * span], part[0, : 2 * span, :], preferred_element_type=jnp.float32
            )
            acc[LOW, :, lt] = jnp.dot(
                wide_v[:tall, :span], part[1, :span, :], preferred_element_type=jnp.float32
            )

    def group(blocks, between=()):
        g = len(blocks)
        depth = g * span
        info = []
        for j, d in enumerate(blocks):
            q, flip = pair_of(d)
            is_low = q < p
            k_low, k_high = halves_of(d, 0, flip)
            v_low, v_high = halves_of(d, 1, flip)
            at_j = slice(j * span, (j + 1) * span)
            wide_v[:head_size, at_j] = v_low.T
            v_x = jnp.where(is_low, v_low, v_high).T
            nil = jnp.zeros_like(v_x)
            wide_v[tall : tall + head_size, at_j] = jnp.where(is_low, v_x, nil)
            wide_v[tall + head_size : 2 * tall, at_j] = jnp.where(is_low, ones, jnp.zeros_like(ones))
            wide_v[2 * tall : 2 * tall + head_size, at_j] = jnp.where(is_low, nil, v_x)
            wide_v[2 * tall + head_size :, at_j] = jnp.where(is_low, jnp.zeros_like(ones), ones)
            info.append((is_low, k_low, jnp.where(is_low, k_low, k_high)))
        for t in range(tiles):
            lt = lane_tile(t)
            old_high = top[HIGH, :, lt]
            old_low = top[LOW, :, lt]
            high, low = old_high, old_low
            base = (t % 2) * 8
            for j, (is_low, k_low, k_x) in enumerate(info):
                s = scores(k_low, HIGH, t)
                raw[base + 2 * j] = s
                high = jnp.maximum(high, peak(s))
                s = scores(k_x, 1 - is_low.astype(jnp.int32), t)
                raw[base + 2 * j + 1] = s
                m = peak(s)
                low = jnp.where(is_low, jnp.maximum(low, m), low)
                high = jnp.where(is_low, high, jnp.maximum(high, m))
            high = spread(high)
            low = spread(low)
            top[HIGH, :, lt] = high
            top[LOW, :, lt] = low
            pb = (t % 2) * 2
            for j, (is_low, _, _) in enumerate(info):
                at_j = slice(j * span, (j + 1) * span)
                part[pb, at_j, :] = weigh(base + 2 * j, high)
                part[pb + 1, at_j, :] = weigh(base + 2 * j + 1, jnp.where(is_low, low, high))
            more = jnp.dot(
                wide_v[:tall, :depth], part[pb, :depth, :], preferred_element_type=jnp.float32
            )
            mixed = jnp.dot(
                wide_v[tall:, :depth], part[pb + 1, :depth, :], preferred_element_type=jnp.float32
            )

            def scaled(which, old, new):
                return (
                    acc[which, :, lt].reshape(tall // 8, 8, tile) * jnp.exp2(old - new)[None]
                ).reshape(tall, tile)

            acc[HIGH, :, lt] = scaled(HIGH, old_high, high) + (more + mixed[tall:])
            acc[LOW, :, lt] = scaled(LOW, old_low, low) + mixed[:tall]
            if t < len(between):
                between[t]()

    own()
    def run(todo):
        for one in todo:
            one()

    def mixed(a, b):
        return [one for pair in zip(a, b) for one in pair]

    run(mixed(events(line_event, 1), events(side_event, 0)))
    from_twin(z, y)
    from_twin(z, far_y)
    group([twin, side, at(z, 1 - y, 1 - c)])
    for r in range(1, zs):
        if r + 1 < zs:
            run(mixed(events(line_event, r + 1), events(side_event, r)))
        else:
            run(events(side_event, r))
        zz = plane(r)
        if r + 1 == zs:
            from_twin(zz, y)
            group([at(zz, y, c), at(zz, y, 1 - c)])
            from_twin(zz, far_y)
            group([at(zz, 1 - y, c), at(zz, 1 - y, 1 - c)])
        else:
            from_twin(zz, y)
            from_twin(zz, far_y)
            group([at(zz, y, c), at(zz, y, 1 - c), at(zz, 1 - y, c), at(zz, 1 - y, 1 - c)])

    all_sent()


def share_kernel(heads, span, order_ref, acc, out_ref):
    head_size = out_ref.shape[1] // heads
    spans = (slice(0, span), slice(span, 2 * span))
    me = lax.axis_index("ctx")
    swapped = order_ref[2 * me + 1] < order_ref[2 * me]
    for h in range(heads):
        cols = slice(h * head_size, (h + 1) * head_size)
        src = slice(h * span, (h + 1) * span)
        outs = []
        for which in (LOW, HIGH):
            total = acc[which, head_size : head_size + 8, src]
            share = acc[which, :head_size, src].reshape(head_size // 8, 8, span) / total[None]
            outs.append(share.reshape(head_size, span).astype(jnp.bfloat16).T)
        out_ref[spans[0], cols] = jnp.where(swapped, outs[HIGH], outs[LOW])
        out_ref[spans[1], cols] = jnp.where(swapped, outs[LOW], outs[HIGH])


def fused(n, queries, keys, values, span_order):
    local_rows, width = queries.shape
    head_size = keys.shape[1]
    heads = width // head_size
    span = local_rows // 2
    rows = heads * span
    anywhere = pl.BlockSpec(memory_space=pltpu.HBM)
    tall = head_size + EXTRA
    vmem = pl.BlockSpec(memory_space=pltpu.VMEM)
    acc = pl.pallas_call(
        functools.partial(fused_kernel, n, heads, span),
        out_shape=jax.ShapeDtypeStruct((2, tall, rows), jnp.float32),
        in_specs=[anywhere, anywhere, anywhere, anywhere],
        out_specs=vmem,
        scratch_shapes=[
            pltpu.SMEM(span_order.shape, jnp.int32),
            pltpu.VMEM((n, 2, local_rows, head_size), jnp.bfloat16),
            pltpu.VMEM((local_rows, width), jnp.bfloat16),
            pltpu.VMEM((2, head_size, rows), jnp.bfloat16),
            pltpu.VMEM((2, 8, rows), jnp.float32),
            pltpu.VMEM((16, span, 2 * span), jnp.float32),
            pltpu.VMEM((4, 4 * span, 2 * span), jnp.bfloat16),
            pltpu.VMEM((3 * tall, 4 * span), jnp.bfloat16),
            pltpu.SemaphoreType.DMA((4,)),
            pltpu.SemaphoreType.DMA((4,)),
            pltpu.SemaphoreType.DMA((n // 4, 2, PIECES)),
            pltpu.SemaphoreType.DMA((n // 4, 2, PIECES)),
            pltpu.SemaphoreType.DMA((n // 4, 2)),
        ],
        compiler_params=pltpu.CompilerParams(
            collective_id=0, has_side_effects=True, vmem_limit_bytes=GRANT
        ),
        name="fused",
    )(*(pltpu.with_memory_space_constraint(x, pltpu.HBM) for x in (span_order, queries, keys, values)))
    return pl.pallas_call(
        functools.partial(share_kernel, heads, span),
        out_shape=jax.ShapeDtypeStruct((local_rows, width), jnp.bfloat16),
        in_specs=[pl.BlockSpec(memory_space=pltpu.SMEM), vmem],
        out_specs=vmem,
        compiler_params=pltpu.CompilerParams(vmem_limit_bytes=GRANT),
        name="share",
    )(span_order, acc)


def body(n, queries, keys, values, span_order):
    if n <= FUSED_MOST:
        return fused(n, queries, keys, values, span_order)
    local_rows, width = queries.shape
    head_size = keys.shape[1]
    heads = width // head_size
    span = local_rows // 2
    vmem = pl.BlockSpec(memory_space=pltpu.VMEM)
    gathered = pl.pallas_call(
        functools.partial(gather_kernel, n),
        out_shape=jax.ShapeDtypeStruct((n, 2, local_rows, head_size), jnp.bfloat16),
        in_specs=[vmem, vmem],
        out_specs=vmem,
        scratch_shapes=[
            pltpu.SemaphoreType.DMA((n, 2, 4)),
            pltpu.SemaphoreType.DMA((n, 2)),
        ],
        compiler_params=pltpu.CompilerParams(collective_id=0, has_side_effects=True),
        name="gather",
    )(keys, values)
    half_keys = n * span
    more_keys = (n + 2) * span
    return pl.pallas_call(
        functools.partial(attend_kernel, n, heads, span),
        out_shape=jax.ShapeDtypeStruct((local_rows, width), jnp.bfloat16),
        in_specs=[vmem, vmem, pl.BlockSpec(memory_space=pltpu.SMEM)],
        out_specs=vmem,
        scratch_shapes=[
            pltpu.VMEM((2, heads, span, head_size), jnp.bfloat16),
            pltpu.VMEM((half_keys, head_size), jnp.bfloat16),
            pltpu.VMEM((half_keys, 2 * head_size), jnp.bfloat16),
            pltpu.VMEM((more_keys, head_size), jnp.bfloat16),
            pltpu.VMEM((more_keys, 2 * head_size), jnp.bfloat16),
            pltpu.VMEM((2, span, half_keys), jnp.float32),
            pltpu.VMEM((2, span, more_keys), jnp.float32),
            pltpu.VMEM((2, span, half_keys), jnp.bfloat16),
            pltpu.VMEM((2, span, more_keys), jnp.bfloat16),
        ],
        name="attend",
    )(queries, gathered, span_order)


def solution(mesh):
    in_specs = (
        P(("groups", "ctx"), None),
        P(("groups", "ctx"), None),
        P(("groups", "ctx"), None),
        P("groups"),
    )
    out_specs = P(("groups", "ctx"), None)
    return jax.shard_map(
        functools.partial(body, mesh.shape["ctx"]),
        mesh=mesh,
        in_specs=in_specs,
        out_specs=out_specs,
        check_vma=False,
    )
```

```python
import functools
import math

import jax
import jax.numpy as jnp
from jax import lax
from jax.experimental import pallas as pl
from jax.experimental.pallas import tpu as pltpu
from jax.sharding import PartitionSpec as P

UP, DOWN, SIDE, TWIN = 0, 1, 2, 3
NEG = -1e30
FUSED_MOST = 32
PIECES = 2
EARLY = ((0, 0), (0, 1), (1, 0))
GRANT = 24 << 20


def gather_kernel(n, k_ref, v_ref, buf, send_sem, recv_sem):
    lanes = 4
    zs = n // lanes
    me = lax.axis_index("ctx")
    z = me // lanes
    lane = lax.rem(me, lanes)
    y = lane // 2
    c = lax.rem(lane, 2)
    side = z * lanes + (1 - y) * 2 + c
    twin = z * lanes + y * 2 + (1 - c)
    not_top = z < zs - 1
    not_bottom = z > 0
    up = jnp.minimum(me + lanes, n - lanes + lane)
    down = jnp.maximum(me - lanes, lane)
    target = (up, down, side, twin)

    barrier = pltpu.get_barrier_semaphore()

    def greet(who):
        pl.semaphore_signal(
            barrier, inc=1, device_id={"ctx": who}, device_id_type=pl.DeviceIdType.MESH
        )

    greet(side)
    greet(twin)
    pl.when(not_top)(lambda: greet(up))
    pl.when(not_bottom)(lambda: greet(down))
    pl.semaphore_wait(barrier, 2 + not_top.astype(jnp.int32) + not_bottom.astype(jnp.int32))

    def copy(block, kv, route, src=None):
        return pltpu.make_async_remote_copy(
            src_ref=buf.at[block, kv] if src is None else src,
            dst_ref=buf.at[block, kv],
            send_sem=send_sem.at[block, kv, route],
            recv_sem=recv_sem.at[block, kv],
            device_id={"ctx": target[route]},
            device_id_type=pl.DeviceIdType.MESH,
        )

    own = (k_ref, v_ref)
    for kv in range(2):
        pl.when(not_top)(lambda: copy(me, kv, UP, own[kv]).start())
        pl.when(not_bottom)(lambda: copy(me, kv, DOWN, own[kv]).start())
        copy(me, kv, SIDE, own[kv]).start()
        copy(me, kv, TWIN, own[kv]).start()
    buf[me, 0] = k_ref[...]
    buf[me, 1] = v_ref[...]

    def at(zz, yy, cc):
        return zz * lanes + yy * 2 + cc

    def from_line(zz, onward, keep):
        block = at(zz, y, c)
        for kv in range(2):
            copy(block, kv, onward).wait_recv()
            pl.when(keep)(lambda: copy(block, kv, onward).start())
            copy(block, kv, SIDE).start()
            copy(block, kv, TWIN).start()

    def from_side(zz):
        block = at(zz, 1 - y, c)
        for kv in range(2):
            copy(block, kv, TWIN).wait_recv()
            copy(block, kv, TWIN).start()

    def from_twin(zz):
        for yy in (y, 1 - y):
            for kv in range(2):
                copy(at(zz, yy, 1 - c), kv, TWIN).wait_recv()

    def both(s, low, high):
        pl.when(z >= s)(lambda: low(z - s))
        pl.when(z + s < zs)(lambda: high(z + s))

    for s in range(1, zs):
        both(s, lambda zz: from_line(zz, UP, not_top), lambda zz: from_line(zz, DOWN, not_bottom))
        if s == 1:
            from_side(z)
        else:
            both(s - 1, from_side, from_side)
    both(zs - 1, from_side, from_side)
    from_twin(z)
    for s in range(1, zs):
        both(s, from_twin, from_twin)

    for kv in range(2):
        pl.when(not_top)(lambda: copy(me, kv, UP, own[kv]).wait_send())
        pl.when(not_bottom)(lambda: copy(me, kv, DOWN, own[kv]).wait_send())
        copy(me, kv, SIDE, own[kv]).wait_send()
        copy(me, kv, TWIN, own[kv]).wait_send()

    def line_sent(zz, onward, keep):
        for kv in range(2):
            pl.when(keep)(lambda: copy(at(zz, y, c), kv, onward).wait_send())
            copy(at(zz, y, c), kv, SIDE).wait_send()
            copy(at(zz, y, c), kv, TWIN).wait_send()

    def side_sent(zz):
        for kv in range(2):
            copy(at(zz, 1 - y, c), kv, TWIN).wait_send()

    side_sent(z)
    for s in range(1, zs):
        both(s, lambda zz: line_sent(zz, UP, not_top), lambda zz: line_sent(zz, DOWN, not_bottom))
        both(s, side_sent, side_sent)


def attend_kernel(
    n, heads, span, q_ref, kv_ref, order_ref, out_ref, qs, k1, v1, k2, v2, raw1, raw2, w1, w2
):
    head_size = k1.shape[1]
    me = lax.axis_index("ctx")
    first = order_ref[2 * me]
    second = order_ref[2 * me + 1]
    p = jnp.minimum(first, second)
    swapped = second < first
    low_at = swapped.astype(jnp.int32)
    pad_high = lax.rem(p, 2)
    pad_low = 1 - pad_high
    chunks_low = (p + 1 + pad_low) // 2
    halves = (slice(0, span), slice(span, 2 * span))

    def rows_of(slot):
        return pl.ds(pl.multiple_of(slot * span, span), span)

    def put(slot, block, half, is_low):
        k2[rows_of(slot), :] = kv_ref[block, 0, rows_of(half), :]
        value = kv_ref[block, 1, rows_of(half), :]
        zero = jnp.zeros_like(value)
        v2[rows_of(slot), :head_size] = jnp.where(is_low, value, zero)
        v2[rows_of(slot), head_size:] = jnp.where(is_low, zero, value)

    put(1, me, low_at, True)
    put(n, me, low_at, False)
    put(0, me, low_at, True)
    put(n + 1, me, 1 - low_at, False)

    def place(d, carry):
        q = jnp.minimum(order_ref[2 * d], order_ref[2 * d + 1])
        lo = (order_ref[2 * d + 1] < order_ref[2 * d]).astype(jnp.int32)
        is_low = q < p

        @pl.when(q != p)
        def _():
            slot = jnp.where(is_low, q + 1 + pad_low, n + 1 - pad_high - (q - p))
            put(slot, d, jnp.where(is_low, lo, 1 - lo), is_low)

        k1[rows_of(d), :] = kv_ref[d, 0, rows_of(lo), :]
        v1[rows_of(d), :head_size] = kv_ref[d, 1, rows_of(lo), :]
        return carry

    lax.fori_loop(0, n, place, 0)
    v1[:, head_size:] = jnp.ones_like(v1[:, head_size:])
    for h in range(heads):
        cols = slice(h * head_size, (h + 1) * head_size)
        pair = [q_ref[s, cols] for s in halves]
        qs[0, h] = jnp.where(swapped, pair[1], pair[0])
        qs[1, h] = jnp.where(swapped, pair[0], pair[1])

    factor = math.log2(math.e) / math.sqrt(head_size)
    ahead = lax.broadcasted_iota(jnp.int32, (span, span), 1) - lax.broadcasted_iota(
        jnp.int32, (span, span), 0
    )
    kept_first = jnp.concatenate([ahead <= 0, ahead <= span - 2 * span * pad_low], axis=1)
    kept_last = jnp.concatenate([ahead <= span - 2 * span * pad_high, ahead <= 0], axis=1)
    chunks1 = n // 2
    chunks2 = n // 2 + 1
    wide = 2 * span

    def scores(q, keys):
        return (
            lax.dot_general(q, keys, (((1,), (1,)), ((), ())), preferred_element_type=jnp.float32)
            * factor
        )

    def folded(x, op):
        return op(x[:, :span], x[:, span:])

    def one_head(h, b):
        high = jnp.full((span, span), NEG, jnp.float32)
        low = high
        for i in range(chunks1):
            cols = slice(i * wide, (i + 1) * wide)
            score = scores(qs[1, h], k1[cols, :])
            raw1[b, :, cols] = score
            high = jnp.maximum(high, folded(score, jnp.maximum))
        for i in range(chunks2):
            cols = slice(i * wide, (i + 1) * wide)
            is_low = i < chunks_low
            score = scores(qs[1 - is_low.astype(jnp.int32), h], k2[cols, :])
            if i == 0:
                score = jnp.where(kept_first, score, NEG)
            if i == chunks2 - 1:
                score = jnp.where(kept_last, score, NEG)
            raw2[b, :, cols] = score
            most = folded(score, jnp.maximum)
            low = jnp.where(is_low, jnp.maximum(low, most), low)
            high = jnp.where(is_low, high, jnp.maximum(high, most))
        low = jnp.broadcast_to(jnp.max(low, axis=1, keepdims=True), (span, span))
        high = jnp.broadcast_to(jnp.max(high, axis=1, keepdims=True), (span, span))
        for i in range(chunks1):
            cols = slice(i * wide, (i + 1) * wide)
            shift = jnp.concatenate([high, high], axis=1)
            w1[b, :, cols] = jnp.exp2(raw1[b, :, cols] - shift).astype(jnp.bfloat16)
        sum_low = jnp.zeros((span, span), jnp.float32)
        sum_high = sum_low
        for i in range(chunks2):
            cols = slice(i * wide, (i + 1) * wide)
            is_low = i < chunks_low
            shift = jnp.where(is_low, low, high)
            weight = jnp.exp2(raw2[b, :, cols] - jnp.concatenate([shift, shift], axis=1))
            w2[b, :, cols] = weight.astype(jnp.bfloat16)
            add = folded(weight, jnp.add)
            sum_low = jnp.where(is_low, sum_low + add, sum_low)
            sum_high = jnp.where(is_low, sum_high, sum_high + add)
        got1 = jnp.dot(w1[b], v1[...], preferred_element_type=jnp.float32)
        got2 = jnp.dot(w2[b], v2[...], preferred_element_type=jnp.float32)
        sum_low = jnp.sum(sum_low, axis=1, keepdims=True)
        sum_high = jnp.sum(sum_high, axis=1, keepdims=True)
        out_low = got2[:, :head_size] / sum_low
        out_high = (got1[:, :head_size] + got2[:, head_size:]) / (got1[:, head_size:] + sum_high)
        cols = pl.ds(pl.multiple_of(h * head_size, head_size), head_size)
        out_ref[halves[0], cols] = jnp.where(swapped, out_high, out_low).astype(jnp.bfloat16)
        out_ref[halves[1], cols] = jnp.where(swapped, out_low, out_high).astype(jnp.bfloat16)

    together = 2 if chunks1 <= heads else 1

    def some_heads(g, carry):
        for b in range(together):
            one_head(g * together + b, b)
        return carry

    lax.fori_loop(0, heads // together, some_heads, 0)


LOW, HIGH = 0, 1
EXTRA = 16


def fused_kernel(
    n, heads, span, order_hbm, q_hbm, k_hbm, v_hbm, out_ref,
    order_ref, buf, q_in, qt, acc, top, raw, part, wide_v, keys_h, keys_x, load_sem, send_sem, line_sem, side_sem, twin_sem,
):
    lanes = 4
    zs = n // lanes
    head_size = buf.shape[3]
    rows = heads * span
    tile = 2 * span
    tiles = rows // tile
    tall = head_size + EXTRA
    me = lax.axis_index("ctx")
    z = me // lanes
    lane = lax.rem(me, lanes)
    y = lane // 2
    c = lax.rem(lane, 2)
    side = z * lanes + (1 - y) * 2 + c
    twin = z * lanes + y * 2 + (1 - c)
    not_top = z < zs - 1
    not_bottom = z > 0
    up = jnp.minimum(me + lanes, n - lanes + lane)
    down = jnp.maximum(me - lanes, lane)
    target = (up, down, side, twin)

    load_k = pltpu.make_async_copy(k_hbm, buf.at[me, 0], load_sem.at[0])
    load_v = pltpu.make_async_copy(v_hbm, buf.at[me, 1], load_sem.at[1])
    load_q = pltpu.make_async_copy(q_hbm, q_in, load_sem.at[2])
    load_order = pltpu.make_async_copy(order_hbm, order_ref, load_sem.at[3])
    load_k.start()
    load_v.start()
    load_order.start()
    load_q.start()

    barrier = pltpu.get_barrier_semaphore()

    def greet(who):
        pl.semaphore_signal(
            barrier, inc=1, device_id={"ctx": who}, device_id_type=pl.DeviceIdType.MESH
        )

    greet(side)
    greet(twin)
    pl.when(not_top)(lambda: greet(up))
    pl.when(not_bottom)(lambda: greet(down))
    load_k.wait()
    load_v.wait()
    pl.semaphore_wait(barrier, 2 + not_top.astype(jnp.int32) + not_bottom.astype(jnp.int32))

    piece = span * 2 // PIECES

    def copy(zz, yy, kv, part_of, route):
        block = at(zz, yy, c)
        where = buf.at[block, kv, pl.ds(part_of * piece, piece)]
        other = yy is not y
        if route == SIDE:
            landed = side_sem.at[zz, kv, part_of]
        elif route == TWIN:
            landed = twin_sem.at[zz, int(other)]
        elif other:
            landed = side_sem.at[zz, kv, part_of]
        else:
            landed = line_sem.at[zz, kv, part_of]
        return pltpu.make_async_remote_copy(
            src_ref=where,
            dst_ref=where,
            send_sem=send_sem.at[route],
            recv_sem=landed,
            device_id={"ctx": target[route]},
            device_id_type=pl.DeviceIdType.MESH,
        )

    def at(zz, yy, cc):
        return zz * lanes + yy * 2 + cc

    far_y = 1 - y
    at_bottom = z == 0
    at_top = z == zs - 1

    def can_be_early(kv, i):
        return zs > 2 and (kv, i) in EARLY

    def early(zz, kv, i):
        if not can_be_early(kv, i):
            return jnp.bool_(False)
        return jnp.logical_or(zz == 0, zz == zs - 1)

    def sends_own(act):
        for kv in range(2):
            for i in range(PIECES):
                pl.when(not_top)(lambda: act(copy(z, y, kv, i, UP)))
                pl.when(not_bottom)(lambda: act(copy(z, y, kv, i, DOWN)))
                act(copy(z, y, kv, i, SIDE))
                act(copy(z, y, kv, i, TWIN))

    def sends_line(zz, kv, i, onward, act):
        pl.when(not_top if onward == UP else not_bottom)(lambda: act(copy(zz, y, kv, i, onward)))
        pl.when(jnp.logical_not(early(zz, kv, i)))(lambda: act(copy(zz, y, kv, i, SIDE)))
        act(copy(zz, y, kv, i, TWIN))

    def sends_side(zz, kv, i, onward, act):
        more = not_top if onward == UP else not_bottom
        if can_be_early(kv, i):
            pl.when(jnp.logical_and(early(zz, kv, i), more))(lambda: act(copy(zz, far_y, kv, i, onward)))
        act(copy(zz, far_y, kv, i, TWIN))

    def sends_near(kv, i, act):
        if can_be_early(kv, i):
            pl.when(at_bottom)(lambda: act(copy(z, far_y, kv, i, UP)))
            pl.when(at_top)(lambda: act(copy(z, far_y, kv, i, DOWN)))
        act(copy(z, far_y, kv, i, TWIN))

    def begin(one):
        one.start()

    def arrived(zz, yy, kv, i):
        where = buf.at[at(zz, yy, c), kv, pl.ds(i * piece, piece)]
        sem = (line_sem if yy is y else side_sem).at[zz, kv, i]
        pltpu.make_async_copy(where, where, sem).wait()

    def both(s, low, high):
        pl.when(z >= s)(lambda: low(z - s))
        pl.when(z + s < zs)(lambda: high(z + s))

    def line_event(s, kv, i):
        def arrive(zz, onward):
            arrived(zz, y, kv, i)
            sends_line(zz, kv, i, onward, begin)

        both(s, lambda zz: arrive(zz, UP), lambda zz: arrive(zz, DOWN))

    def side_event(s, kv, i):
        def arrive(zz, onward):
            arrived(zz, far_y, kv, i)
            sends_side(zz, kv, i, onward, begin)

        if s:
            both(s, lambda zz: arrive(zz, UP), lambda zz: arrive(zz, DOWN))
        else:
            arrived(z, far_y, kv, i)
            sends_near(kv, i, begin)

    def events(kind, s):
        return [functools.partial(kind, s, kv, i) for kv in range(2) for i in range(PIECES)]

    def from_twin(zz, yy):
        where = buf.at[at(zz, yy, 1 - c)]
        pltpu.make_async_copy(where, where, twin_sem.at[zz, int(yy is not y)]).wait()

    def all_sent():
        def taken(pieces, route):
            if pieces % (2 * PIECES) == 0:
                where = buf.at[pl.ds(0, pieces // (2 * PIECES))]
            else:
                where = buf.at[0, pl.ds(0, 2), pl.ds(0, pieces * piece // 2)]
            pltpu.make_async_copy(where, where, send_sem.at[route]).wait()

        whole = 2 * PIECES
        few = len(EARLY) if zs > 2 else 0
        taken(2 * zs * whole, TWIN)
        taken(whole, SIDE)
        for zz in range(zs):
            kept_back = few if zz in (0, zs - 1) else 0
            if whole > kept_back:
                pl.when(zz != z)(lambda: taken(whole - kept_back, SIDE))
            pl.when(jnp.logical_and(not_top, zz <= z))(lambda: taken(whole, UP))
            pl.when(jnp.logical_and(not_bottom, zz >= z))(lambda: taken(whole, DOWN))
        if few:
            pl.when(not_top)(lambda: taken(few, UP))
            pl.when(not_bottom)(lambda: taken(few, DOWN))

    sends_own(begin)

    inner = jnp.minimum(z, zs - 1 - z)
    outward = jnp.where(z < zs - 1 - z, 1, -1)

    def plane(r):
        near = z + ((r + 1) // 2) * (1 if r % 2 == 0 else -1)
        return jnp.where(r <= 2 * inner, near, z + (r - inner) * outward)

    def pair_of(d):
        first = order_ref[2 * d]
        second = order_ref[2 * d + 1]
        return jnp.minimum(first, second), second < first

    load_order.wait()
    p, swapped = pair_of(me)
    factor = math.log2(math.e) / math.sqrt(head_size)
    spans = (slice(0, span), slice(span, 2 * span))

    load_q.wait()
    for h in range(heads):
        cols = slice(h * head_size, (h + 1) * head_size)
        dest = slice(h * span, (h + 1) * span)
        a = q_in[spans[0], cols]
        b = q_in[spans[1], cols]
        qt[LOW, :, dest] = jnp.where(swapped, b, a).T
        qt[HIGH, :, dest] = jnp.where(swapped, a, b).T

    def lane_tile(t):
        return slice(t * tile, (t + 1) * tile)

    def peak(score):
        return jnp.max(score.reshape(span // 8, 8, tile), axis=0)

    def spread(m):
        return jnp.broadcast_to(jnp.max(m, axis=0, keepdims=True), (8, tile))

    def halves_of(d, kv, flip):
        a = buf[d, kv, spans[0], :]
        b = buf[d, kv, spans[1], :]
        return jnp.where(flip, b, a), jnp.where(flip, a, b)

    def nth(j):
        return slice(j * span, (j + 1) * span)

    kept = lax.broadcasted_iota(jnp.int32, (span, tile), 0) <= lax.rem(
        lax.broadcasted_iota(jnp.int32, (span, tile), 1), span
    )
    ones = jnp.ones((EXTRA, span), jnp.bfloat16)
    wide_v[head_size:tall, :] = jnp.ones_like(wide_v[head_size:tall, :])

    def group(blocks, first=False, final=False):
        high_masks, x_units = [], []

        def add_high(keys, masked):
            keys_h[nth(len(high_masks)), :] = keys
            high_masks.append(masked)

        def add_x(keys, is_low, masked):
            keys_x[nth(len(x_units)), :] = keys
            x_units.append((is_low, masked))

        def values_high(j, values):
            wide_v[:head_size, nth(j)] = values.T

        def values_x(j, values):
            is_low = x_units[j][0]
            at_j = nth(j)
            turned = values.T
            nil, none = jnp.zeros_like(turned), jnp.zeros_like(ones)
            if is_low is True:
                parts = (turned, ones, nil, none)
            else:
                parts = (
                    jnp.where(is_low, turned, nil),
                    jnp.where(is_low, ones, none),
                    jnp.where(is_low, nil, turned),
                    jnp.where(is_low, none, ones),
                )
            wide_v[tall : tall + head_size, at_j] = parts[0]
            wide_v[tall + head_size : 2 * tall, at_j] = parts[1]
            wide_v[2 * tall : 2 * tall + head_size, at_j] = parts[2]
            wide_v[2 * tall + head_size :, at_j] = parts[3]

        if first:
            k_low, k_high = halves_of(me, 0, swapped)
            add_high(k_low, False)
            add_high(k_high, True)
            add_x(k_low, True, True)
        for d in blocks:
            q, flip = pair_of(d)
            is_low = q < p
            k_low, k_high = halves_of(d, 0, flip)
            add_high(k_low, False)
            add_x(jnp.where(is_low, k_low, k_high), is_low, False)

        def turn_values():
            high, x = 0, 0
            if first:
                v_low, v_high = halves_of(me, 1, swapped)
                values_high(0, v_low)
                values_high(1, v_high)
                values_x(0, v_low)
                high, x = 2, 1
            for j, d in enumerate(blocks):
                v_low, v_high = halves_of(d, 1, pair_of(d)[1])
                values_high(high + j, v_low)
                values_x(x + j, jnp.where(x_units[x + j][0], v_low, v_high))

        turn_values()
        n_high, n_x = len(high_masks), len(x_units)
        units = n_high + n_x

        def base(t):
            return t * units if final else (t % 2) * 8

        def weights_at(t, of_x):
            if final:
                return t, of_x * n_high * span
            return (t % 2) * 2 + of_x, 0

        peaks = {}

        def start_tile(t):
            lt = lane_tile(t)
            if first:
                low = high = jnp.full((8, tile), NEG, jnp.float32)
            else:
                high, low = top[HIGH, :, lt], top[LOW, :, lt]
            peaks[t] = [high, low, high, low]

        def score_steps(t):
            lt = lane_tile(t)

            def of_high(lo, hi):
                found = jnp.dot(
                    keys_h[lo * span : hi * span, :], qt[HIGH, :, lt], preferred_element_type=jnp.float32
                )
                for u in range(lo, hi):
                    s = found[nth(u - lo)]
                    if high_masks[u]:
                        s = jnp.where(kept, s, NEG)
                    raw[base(t) + u] = s
                    peaks[t][2] = jnp.maximum(peaks[t][2], peak(s))

            def of_x(u):
                is_low, masked = x_units[u]
                which = LOW if is_low is True else 1 - is_low.astype(jnp.int32)
                s = jnp.dot(keys_x[nth(u), :], qt[which, :, lt], preferred_element_type=jnp.float32)
                if masked:
                    s = jnp.where(kept, s, NEG)
                raw[base(t) + n_high + u] = s
                m = peak(s)
                if is_low is True:
                    peaks[t][3] = jnp.maximum(peaks[t][3], m)
                else:
                    peaks[t][3] = jnp.where(is_low, jnp.maximum(peaks[t][3], m), peaks[t][3])
                    peaks[t][2] = jnp.where(is_low, peaks[t][2], jnp.maximum(peaks[t][2], m))

            steps = [
                functools.partial(of_high, lo, min(lo + 2, n_high)) for lo in range(0, n_high, 2)
            ]
            return steps + [functools.partial(of_x, u) for u in range(n_x)]

        def end_tile(t):
            lt = lane_tile(t)
            peaks[t][2:] = [spread(peaks[t][2]), spread(peaks[t][3])]
            top[HIGH, :, lt] = peaks[t][2]
            top[LOW, :, lt] = peaks[t][3]

        def weigh_steps(t):
            def weigh(u):
                if u < n_high:
                    m, row = peaks[t][2], u
                else:
                    is_low = x_units[u - n_high][0]
                    m = peaks[t][3] if is_low is True else jnp.where(is_low, peaks[t][3], peaks[t][2])
                    row = u - n_high
                dest, start = weights_at(t, int(u >= n_high))
                s = raw[base(t) + u].reshape(span // 8, 8, tile)
                w = jnp.exp2((s - m[None]) * factor)
                part[dest, start + row * span : start + (row + 1) * span, :] = w.reshape(span, tile).astype(jnp.bfloat16)

            return [functools.partial(weigh, u) for u in range(units)]

        def gather_values(t):
            lt = lane_tile(t)
            a, a0 = weights_at(t, 0)
            b, b0 = weights_at(t, 1)
            more = jnp.dot(
                wide_v[:tall, : n_high * span],
                part[a, a0 : a0 + n_high * span, :],
                preferred_element_type=jnp.float32,
            )
            both_rows = jnp.dot(
                wide_v[tall:, : n_x * span],
                part[b, b0 : b0 + n_x * span, :],
                preferred_element_type=jnp.float32,
            )
            if first:
                acc[HIGH, :, lt] = more + both_rows[tall:]
                acc[LOW, :, lt] = both_rows[:tall]
                return

            def scaled(which, old, new):
                shrink = jnp.exp2((old - new) * factor)
                return (acc[which, :, lt].reshape(tall // 8, 8, tile) * shrink[None]).reshape(tall, tile)

            high = scaled(HIGH, peaks[t][0], peaks[t][2]) + (more + both_rows[tall:])
            low = scaled(LOW, peaks[t][1], peaks[t][3]) + both_rows[:tall]
            if not final:
                acc[HIGH, :, lt] = high
                acc[LOW, :, lt] = low
                return
            rows_of = []
            for whole in (low, high):
                total = jnp.float32(1.0) / whole[head_size : head_size + 8]
                share = whole[:head_size].reshape(head_size // 8, 8, tile) * total[None]
                rows_of.append(share.reshape(head_size, tile).astype(jnp.bfloat16))
            for k in range(tile // span):
                low_rows, high_rows = (one[:, nth(k)].T for one in rows_of)
                cols = slice((t * (tile // span) + k) * head_size, (t * (tile // span) + k + 1) * head_size)
                out_ref[spans[0], cols] = jnp.where(swapped, high_rows, low_rows)
                out_ref[spans[1], cols] = jnp.where(swapped, low_rows, high_rows)

        start_tile(0)
        for step in score_steps(0):
            step()
        end_tile(0)
        for t in range(tiles):
            ahead = []
            if t + 1 < tiles:
                start_tile(t + 1)
                ahead = score_steps(t + 1)
            now = weigh_steps(t)
            for k in range(max(len(ahead), len(now))):
                if k < len(ahead):
                    ahead[k]()
                if k < len(now):
                    now[k]()
            if not final:
                gather_values(t)
            if t + 1 < tiles:
                end_tile(t + 1)
        if final:
            for t in range(tiles):
                gather_values(t)

    def run(todo):
        for one in todo:
            one()

    def mixed(a, b):
        return [one for pair in zip(a, b) for one in pair]

    def pair(r, yy):
        from_twin(plane(r), yy)
        return [at(plane(r), yy, c), at(plane(r), yy, 1 - c)]

    from_twin(z, y)
    group([twin], first=True)
    run(mixed(events(line_event, 1), events(side_event, 0)))
    for r in range(zs - 1):
        group(pair(r, far_y) + pair(r + 1, y))
        if r + 2 < zs:
            run(mixed(events(line_event, r + 2), events(side_event, r + 1)))
        else:
            run(events(side_event, r + 1))
    group(pair(zs - 1, far_y), final=True)
    all_sent()


def fused(n, queries, keys, values, span_order):
    local_rows, width = queries.shape
    head_size = keys.shape[1]
    heads = width // head_size
    span = local_rows // 2
    rows = heads * span
    anywhere = pl.BlockSpec(memory_space=pltpu.HBM)
    tall = head_size + EXTRA
    vmem = pl.BlockSpec(memory_space=pltpu.VMEM)
    return pl.pallas_call(
        functools.partial(fused_kernel, n, heads, span),
        out_shape=jax.ShapeDtypeStruct((local_rows, width), jnp.bfloat16),
        in_specs=[anywhere, anywhere, anywhere, anywhere],
        out_specs=vmem,
        scratch_shapes=[
            pltpu.SMEM(span_order.shape, jnp.int32),
            pltpu.VMEM((n, 2, local_rows, head_size), jnp.bfloat16),
            pltpu.VMEM((local_rows, width), jnp.bfloat16),
            pltpu.VMEM((2, head_size, rows), jnp.bfloat16),
            pltpu.VMEM((2, tall, rows), jnp.float32),
            pltpu.VMEM((2, 8, rows), jnp.float32),
            pltpu.VMEM((16, span, 2 * span), jnp.float32),
            pltpu.VMEM((4, 4 * span, 2 * span), jnp.bfloat16),
            pltpu.VMEM((3 * tall, 4 * span), jnp.bfloat16),
            pltpu.VMEM((4 * span, head_size), jnp.bfloat16),
            pltpu.VMEM((4 * span, head_size), jnp.bfloat16),
            pltpu.SemaphoreType.DMA((4,)),
            pltpu.SemaphoreType.DMA((4,)),
            pltpu.SemaphoreType.DMA((n // 4, 2, PIECES)),
            pltpu.SemaphoreType.DMA((n // 4, 2, PIECES)),
            pltpu.SemaphoreType.DMA((n // 4, 2)),
        ],
        compiler_params=pltpu.CompilerParams(
            collective_id=0, has_side_effects=True, vmem_limit_bytes=GRANT
        ),
        name="fused",
    )(*(pltpu.with_memory_space_constraint(x, pltpu.HBM) for x in (span_order, queries, keys, values)))


def body(n, queries, keys, values, span_order):
    if n <= FUSED_MOST:
        return fused(n, queries, keys, values, span_order)
    local_rows, width = queries.shape
    head_size = keys.shape[1]
    heads = width // head_size
    span = local_rows // 2
    vmem = pl.BlockSpec(memory_space=pltpu.VMEM)
    gathered = pl.pallas_call(
        functools.partial(gather_kernel, n),
        out_shape=jax.ShapeDtypeStruct((n, 2, local_rows, head_size), jnp.bfloat16),
        in_specs=[vmem, vmem],
        out_specs=vmem,
        scratch_shapes=[
            pltpu.SemaphoreType.DMA((n, 2, 4)),
            pltpu.SemaphoreType.DMA((n, 2)),
        ],
        compiler_params=pltpu.CompilerParams(collective_id=0, has_side_effects=True),
        name="gather",
    )(keys, values)
    half_keys = n * span
    more_keys = (n + 2) * span
    return pl.pallas_call(
        functools.partial(attend_kernel, n, heads, span),
        out_shape=jax.ShapeDtypeStruct((local_rows, width), jnp.bfloat16),
        in_specs=[vmem, vmem, pl.BlockSpec(memory_space=pltpu.SMEM)],
        out_specs=vmem,
        scratch_shapes=[
            pltpu.VMEM((2, heads, span, head_size), jnp.bfloat16),
            pltpu.VMEM((half_keys, head_size), jnp.bfloat16),
            pltpu.VMEM((half_keys, 2 * head_size), jnp.bfloat16),
            pltpu.VMEM((more_keys, head_size), jnp.bfloat16),
            pltpu.VMEM((more_keys, 2 * head_size), jnp.bfloat16),
            pltpu.VMEM((2, span, half_keys), jnp.float32),
            pltpu.VMEM((2, span, more_keys), jnp.float32),
            pltpu.VMEM((2, span, half_keys), jnp.bfloat16),
            pltpu.VMEM((2, span, more_keys), jnp.bfloat16),
        ],
        name="attend",
    )(queries, gathered, span_order)


def solution(mesh):
    in_specs = (
        P(("groups", "ctx"), None),
        P(("groups", "ctx"), None),
        P(("groups", "ctx"), None),
        P("groups"),
    )
    out_specs = P(("groups", "ctx"), None)
    return jax.shard_map(
        functools.partial(body, mesh.shape["ctx"]),
        mesh=mesh,
        in_specs=in_specs,
        out_specs=out_specs,
        check_vma=False,
    )
```

```python
import functools
import math

import jax
import jax.numpy as jnp
from jax import lax
from jax.experimental import pallas as pl
from jax.experimental.pallas import tpu as pltpu
from jax.sharding import PartitionSpec as P

UP, DOWN, SIDE, TWIN = 0, 1, 2, 3
NEG = -1e30
FUSED_MOST = 32
PIECES = 2
EARLY = ((0, 0), (0, 1), (1, 0))
GRANT = 24 << 20


def gather_kernel(n, k_ref, v_ref, buf, send_sem, recv_sem):
    lanes = 4
    zs = n // lanes
    me = lax.axis_index("ctx")
    z = me // lanes
    lane = lax.rem(me, lanes)
    y = lane // 2
    c = lax.rem(lane, 2)
    side = z * lanes + (1 - y) * 2 + c
    twin = z * lanes + y * 2 + (1 - c)
    not_top = z < zs - 1
    not_bottom = z > 0
    up = jnp.minimum(me + lanes, n - lanes + lane)
    down = jnp.maximum(me - lanes, lane)
    target = (up, down, side, twin)

    barrier = pltpu.get_barrier_semaphore()

    def greet(who):
        pl.semaphore_signal(
            barrier, inc=1, device_id={"ctx": who}, device_id_type=pl.DeviceIdType.MESH
        )

    greet(side)
    greet(twin)
    pl.when(not_top)(lambda: greet(up))
    pl.when(not_bottom)(lambda: greet(down))
    pl.semaphore_wait(barrier, 2 + not_top.astype(jnp.int32) + not_bottom.astype(jnp.int32))

    def copy(block, kv, route, src=None):
        return pltpu.make_async_remote_copy(
            src_ref=buf.at[block, kv] if src is None else src,
            dst_ref=buf.at[block, kv],
            send_sem=send_sem.at[block, kv, route],
            recv_sem=recv_sem.at[block, kv],
            device_id={"ctx": target[route]},
            device_id_type=pl.DeviceIdType.MESH,
        )

    own = (k_ref, v_ref)
    for kv in range(2):
        pl.when(not_top)(lambda: copy(me, kv, UP, own[kv]).start())
        pl.when(not_bottom)(lambda: copy(me, kv, DOWN, own[kv]).start())
        copy(me, kv, SIDE, own[kv]).start()
        copy(me, kv, TWIN, own[kv]).start()
    buf[me, 0] = k_ref[...]
    buf[me, 1] = v_ref[...]

    def at(zz, yy, cc):
        return zz * lanes + yy * 2 + cc

    def from_line(zz, onward, keep):
        block = at(zz, y, c)
        for kv in range(2):
            copy(block, kv, onward).wait_recv()
            pl.when(keep)(lambda: copy(block, kv, onward).start())
            copy(block, kv, SIDE).start()
            copy(block, kv, TWIN).start()

    def from_side(zz):
        block = at(zz, 1 - y, c)
        for kv in range(2):
            copy(block, kv, TWIN).wait_recv()
            copy(block, kv, TWIN).start()

    def from_twin(zz):
        for yy in (y, 1 - y):
            for kv in range(2):
                copy(at(zz, yy, 1 - c), kv, TWIN).wait_recv()

    def both(s, low, high):
        pl.when(z >= s)(lambda: low(z - s))
        pl.when(z + s < zs)(lambda: high(z + s))

    for s in range(1, zs):
        both(s, lambda zz: from_line(zz, UP, not_top), lambda zz: from_line(zz, DOWN, not_bottom))
        if s == 1:
            from_side(z)
        else:
            both(s - 1, from_side, from_side)
    both(zs - 1, from_side, from_side)
    from_twin(z)
    for s in range(1, zs):
        both(s, from_twin, from_twin)

    for kv in range(2):
        pl.when(not_top)(lambda: copy(me, kv, UP, own[kv]).wait_send())
        pl.when(not_bottom)(lambda: copy(me, kv, DOWN, own[kv]).wait_send())
        copy(me, kv, SIDE, own[kv]).wait_send()
        copy(me, kv, TWIN, own[kv]).wait_send()

    def line_sent(zz, onward, keep):
        for kv in range(2):
            pl.when(keep)(lambda: copy(at(zz, y, c), kv, onward).wait_send())
            copy(at(zz, y, c), kv, SIDE).wait_send()
            copy(at(zz, y, c), kv, TWIN).wait_send()

    def side_sent(zz):
        for kv in range(2):
            copy(at(zz, 1 - y, c), kv, TWIN).wait_send()

    side_sent(z)
    for s in range(1, zs):
        both(s, lambda zz: line_sent(zz, UP, not_top), lambda zz: line_sent(zz, DOWN, not_bottom))
        both(s, side_sent, side_sent)


def attend_kernel(
    n, heads, span, q_ref, kv_ref, order_ref, out_ref, qs, k1, v1, k2, v2, raw1, raw2, w1, w2
):
    head_size = k1.shape[1]
    me = lax.axis_index("ctx")
    first = order_ref[2 * me]
    second = order_ref[2 * me + 1]
    p = jnp.minimum(first, second)
    swapped = second < first
    low_at = swapped.astype(jnp.int32)
    pad_high = lax.rem(p, 2)
    pad_low = 1 - pad_high
    chunks_low = (p + 1 + pad_low) // 2
    halves = (slice(0, span), slice(span, 2 * span))

    def rows_of(slot):
        return pl.ds(pl.multiple_of(slot * span, span), span)

    def put(slot, block, half, is_low):
        k2[rows_of(slot), :] = kv_ref[block, 0, rows_of(half), :]
        value = kv_ref[block, 1, rows_of(half), :]
        zero = jnp.zeros_like(value)
        v2[rows_of(slot), :head_size] = jnp.where(is_low, value, zero)
        v2[rows_of(slot), head_size:] = jnp.where(is_low, zero, value)

    put(1, me, low_at, True)
    put(n, me, low_at, False)
    put(0, me, low_at, True)
    put(n + 1, me, 1 - low_at, False)

    def place(d, carry):
        q = jnp.minimum(order_ref[2 * d], order_ref[2 * d + 1])
        lo = (order_ref[2 * d + 1] < order_ref[2 * d]).astype(jnp.int32)
        is_low = q < p

        @pl.when(q != p)
        def _():
            slot = jnp.where(is_low, q + 1 + pad_low, n + 1 - pad_high - (q - p))
            put(slot, d, jnp.where(is_low, lo, 1 - lo), is_low)

        k1[rows_of(d), :] = kv_ref[d, 0, rows_of(lo), :]
        v1[rows_of(d), :head_size] = kv_ref[d, 1, rows_of(lo), :]
        return carry

    lax.fori_loop(0, n, place, 0)
    v1[:, head_size:] = jnp.ones_like(v1[:, head_size:])
    for h in range(heads):
        cols = slice(h * head_size, (h + 1) * head_size)
        pair = [q_ref[s, cols] for s in halves]
        qs[0, h] = jnp.where(swapped, pair[1], pair[0])
        qs[1, h] = jnp.where(swapped, pair[0], pair[1])

    factor = math.log2(math.e) / math.sqrt(head_size)
    ahead = lax.broadcasted_iota(jnp.int32, (span, span), 1) - lax.broadcasted_iota(
        jnp.int32, (span, span), 0
    )
    kept_first = jnp.concatenate([ahead <= 0, ahead <= span - 2 * span * pad_low], axis=1)
    kept_last = jnp.concatenate([ahead <= span - 2 * span * pad_high, ahead <= 0], axis=1)
    chunks1 = n // 2
    chunks2 = n // 2 + 1
    wide = 2 * span

    def scores(q, keys):
        return (
            lax.dot_general(q, keys, (((1,), (1,)), ((), ())), preferred_element_type=jnp.float32)
            * factor
        )

    def folded(x, op):
        return op(x[:, :span], x[:, span:])

    def one_head(h, b):
        high = jnp.full((span, span), NEG, jnp.float32)
        low = high
        for i in range(chunks1):
            cols = slice(i * wide, (i + 1) * wide)
            score = scores(qs[1, h], k1[cols, :])
            raw1[b, :, cols] = score
            high = jnp.maximum(high, folded(score, jnp.maximum))
        for i in range(chunks2):
            cols = slice(i * wide, (i + 1) * wide)
            is_low = i < chunks_low
            score = scores(qs[1 - is_low.astype(jnp.int32), h], k2[cols, :])
            if i == 0:
                score = jnp.where(kept_first, score, NEG)
            if i == chunks2 - 1:
                score = jnp.where(kept_last, score, NEG)
            raw2[b, :, cols] = score
            most = folded(score, jnp.maximum)
            low = jnp.where(is_low, jnp.maximum(low, most), low)
            high = jnp.where(is_low, high, jnp.maximum(high, most))
        low = jnp.broadcast_to(jnp.max(low, axis=1, keepdims=True), (span, span))
        high = jnp.broadcast_to(jnp.max(high, axis=1, keepdims=True), (span, span))
        for i in range(chunks1):
            cols = slice(i * wide, (i + 1) * wide)
            shift = jnp.concatenate([high, high], axis=1)
            w1[b, :, cols] = jnp.exp2(raw1[b, :, cols] - shift).astype(jnp.bfloat16)
        sum_low = jnp.zeros((span, span), jnp.float32)
        sum_high = sum_low
        for i in range(chunks2):
            cols = slice(i * wide, (i + 1) * wide)
            is_low = i < chunks_low
            shift = jnp.where(is_low, low, high)
            weight = jnp.exp2(raw2[b, :, cols] - jnp.concatenate([shift, shift], axis=1))
            w2[b, :, cols] = weight.astype(jnp.bfloat16)
            add = folded(weight, jnp.add)
            sum_low = jnp.where(is_low, sum_low + add, sum_low)
            sum_high = jnp.where(is_low, sum_high, sum_high + add)
        got1 = jnp.dot(w1[b], v1[...], preferred_element_type=jnp.float32)
        got2 = jnp.dot(w2[b], v2[...], preferred_element_type=jnp.float32)
        sum_low = jnp.sum(sum_low, axis=1, keepdims=True)
        sum_high = jnp.sum(sum_high, axis=1, keepdims=True)
        out_low = got2[:, :head_size] / sum_low
        out_high = (got1[:, :head_size] + got2[:, head_size:]) / (got1[:, head_size:] + sum_high)
        cols = pl.ds(pl.multiple_of(h * head_size, head_size), head_size)
        out_ref[halves[0], cols] = jnp.where(swapped, out_high, out_low).astype(jnp.bfloat16)
        out_ref[halves[1], cols] = jnp.where(swapped, out_low, out_high).astype(jnp.bfloat16)

    together = 2 if chunks1 <= heads else 1

    def some_heads(g, carry):
        for b in range(together):
            one_head(g * together + b, b)
        return carry

    lax.fori_loop(0, heads // together, some_heads, 0)


LOW, HIGH = 0, 1
EXTRA = 16


def fused_kernel(
    n, heads, span, order_hbm, q_hbm, k_hbm, v_hbm, out_ref,
    order_ref, buf, q_in, qt, acc, top, raw, part, wide_v, keys_h, keys_x, load_sem, send_sem, line_sem, side_sem, twin_sem,
):
    lanes = 4
    zs = n // lanes
    head_size = buf.shape[3]
    rows = heads * span
    tile = 2 * span
    tiles = rows // tile
    tall = head_size + EXTRA
    me = lax.axis_index("ctx")
    z = me // lanes
    lane = lax.rem(me, lanes)
    y = lane // 2
    c = lax.rem(lane, 2)
    side = z * lanes + (1 - y) * 2 + c
    twin = z * lanes + y * 2 + (1 - c)
    not_top = z < zs - 1
    not_bottom = z > 0
    up = jnp.minimum(me + lanes, n - lanes + lane)
    down = jnp.maximum(me - lanes, lane)
    target = (up, down, side, twin)

    load_k = pltpu.make_async_copy(k_hbm, buf.at[me, 0], load_sem.at[0])
    load_v = pltpu.make_async_copy(v_hbm, buf.at[me, 1], load_sem.at[1])
    load_q = pltpu.make_async_copy(q_hbm, q_in, load_sem.at[2])
    load_order = pltpu.make_async_copy(order_hbm, order_ref, load_sem.at[3])
    load_k.start()
    load_v.start()
    load_order.start()
    load_q.start()

    barrier = pltpu.get_barrier_semaphore()

    def greet(who):
        pl.semaphore_signal(
            barrier, inc=1, device_id={"ctx": who}, device_id_type=pl.DeviceIdType.MESH
        )

    greet(side)
    greet(twin)
    pl.when(not_top)(lambda: greet(up))
    pl.when(not_bottom)(lambda: greet(down))
    load_k.wait()
    load_v.wait()
    pl.semaphore_wait(barrier, 2 + not_top.astype(jnp.int32) + not_bottom.astype(jnp.int32))

    piece = span * 2 // PIECES

    def copy(zz, yy, kv, part_of, route):
        block = at(zz, yy, c)
        where = buf.at[block, kv, pl.ds(part_of * piece, piece)]
        other = yy is not y
        if route == SIDE:
            landed = side_sem.at[zz, kv, part_of]
        elif route == TWIN:
            landed = twin_sem.at[zz, int(other)]
        elif other:
            landed = side_sem.at[zz, kv, part_of]
        else:
            landed = line_sem.at[zz, kv, part_of]
        return pltpu.make_async_remote_copy(
            src_ref=where,
            dst_ref=where,
            send_sem=send_sem.at[0],
            recv_sem=landed,
            device_id={"ctx": target[route]},
            device_id_type=pl.DeviceIdType.MESH,
        )

    def at(zz, yy, cc):
        return zz * lanes + yy * 2 + cc

    far_y = 1 - y
    at_bottom = z == 0
    at_top = z == zs - 1

    def can_be_early(kv, i):
        return zs > 2 and (kv, i) in EARLY

    def early(zz, kv, i):
        if not can_be_early(kv, i):
            return jnp.bool_(False)
        return jnp.logical_or(zz == 0, zz == zs - 1)

    def sends_own(act):
        for kv in range(2):
            for i in range(PIECES):
                pl.when(not_top)(lambda: act(copy(z, y, kv, i, UP)))
                pl.when(not_bottom)(lambda: act(copy(z, y, kv, i, DOWN)))
                act(copy(z, y, kv, i, SIDE))
                act(copy(z, y, kv, i, TWIN))

    def sends_line(zz, kv, i, onward, act):
        pl.when(not_top if onward == UP else not_bottom)(lambda: act(copy(zz, y, kv, i, onward)))
        pl.when(jnp.logical_not(early(zz, kv, i)))(lambda: act(copy(zz, y, kv, i, SIDE)))
        act(copy(zz, y, kv, i, TWIN))

    def sends_side(zz, kv, i, onward, act):
        more = not_top if onward == UP else not_bottom
        if can_be_early(kv, i):
            pl.when(jnp.logical_and(early(zz, kv, i), more))(lambda: act(copy(zz, far_y, kv, i, onward)))
        act(copy(zz, far_y, kv, i, TWIN))

    def sends_near(kv, i, act):
        if can_be_early(kv, i):
            pl.when(at_bottom)(lambda: act(copy(z, far_y, kv, i, UP)))
            pl.when(at_top)(lambda: act(copy(z, far_y, kv, i, DOWN)))
        act(copy(z, far_y, kv, i, TWIN))

    def begin(one):
        one.start()

    def arrived(zz, yy, kv, i):
        where = buf.at[at(zz, yy, c), kv, pl.ds(i * piece, piece)]
        sem = (line_sem if yy is y else side_sem).at[zz, kv, i]
        pltpu.make_async_copy(where, where, sem).wait()

    def both(s, low, high):
        pl.when(z >= s)(lambda: low(z - s))
        pl.when(z + s < zs)(lambda: high(z + s))

    def line_event(s, kv, i):
        def arrive(zz, onward):
            arrived(zz, y, kv, i)
            sends_line(zz, kv, i, onward, begin)

        both(s, lambda zz: arrive(zz, UP), lambda zz: arrive(zz, DOWN))

    def side_event(s, kv, i):
        def arrive(zz, onward):
            arrived(zz, far_y, kv, i)
            sends_side(zz, kv, i, onward, begin)

        if s:
            both(s, lambda zz: arrive(zz, UP), lambda zz: arrive(zz, DOWN))
        else:
            arrived(z, far_y, kv, i)
            sends_near(kv, i, begin)

    def events(kind, s):
        return [functools.partial(kind, s, kv, i) for kv in range(2) for i in range(PIECES)]

    def from_twin(zz, yy):
        where = buf.at[at(zz, yy, 1 - c)]
        pltpu.make_async_copy(where, where, twin_sem.at[zz, int(yy is not y)]).wait()

    def all_sent():
        def taken(pieces, route):
            if pieces % (2 * PIECES) == 0:
                where = buf.at[pl.ds(0, pieces // (2 * PIECES))]
            else:
                where = buf.at[0, pl.ds(0, 2), pl.ds(0, pieces * piece // 2)]
            pltpu.make_async_copy(where, where, send_sem.at[0]).wait()

        whole = 2 * PIECES
        few = len(EARLY) if zs > 2 else 0
        taken(2 * zs * whole, TWIN)
        taken(whole, SIDE)
        for zz in range(zs):
            kept_back = few if zz in (0, zs - 1) else 0
            if whole > kept_back:
                pl.when(zz != z)(lambda: taken(whole - kept_back, SIDE))
            pl.when(jnp.logical_and(not_top, zz <= z))(lambda: taken(whole, UP))
            pl.when(jnp.logical_and(not_bottom, zz >= z))(lambda: taken(whole, DOWN))
        if few:
            pl.when(not_top)(lambda: taken(few, UP))
            pl.when(not_bottom)(lambda: taken(few, DOWN))

    sends_own(begin)

    inner = jnp.minimum(z, zs - 1 - z)
    outward = jnp.where(z < zs - 1 - z, 1, -1)

    def plane(r):
        near = z + ((r + 1) // 2) * (1 if r % 2 == 0 else -1)
        return jnp.where(r <= 2 * inner, near, z + (r - inner) * outward)

    def pair_of(d):
        first = order_ref[2 * d]
        second = order_ref[2 * d + 1]
        return jnp.minimum(first, second), second < first

    load_order.wait()
    p, swapped = pair_of(me)
    factor = math.log2(math.e) / math.sqrt(head_size)
    spans = (slice(0, span), slice(span, 2 * span))

    load_q.wait()
    for h in range(heads):
        cols = slice(h * head_size, (h + 1) * head_size)
        dest = slice(h * span, (h + 1) * span)
        a = q_in[spans[0], cols]
        b = q_in[spans[1], cols]
        qt[LOW, :, dest] = jnp.where(swapped, b, a).T
        qt[HIGH, :, dest] = jnp.where(swapped, a, b).T

    def lane_tile(t):
        return slice(t * tile, (t + 1) * tile)

    def peak(score):
        return jnp.max(score.reshape(span // 8, 8, tile), axis=0)

    def spread(m):
        return jnp.broadcast_to(jnp.max(m, axis=0, keepdims=True), (8, tile))

    def halves_of(d, kv, flip):
        a = buf[d, kv, spans[0], :]
        b = buf[d, kv, spans[1], :]
        return jnp.where(flip, b, a), jnp.where(flip, a, b)

    def nth(j):
        return slice(j * span, (j + 1) * span)

    kept = lax.broadcasted_iota(jnp.int32, (span, tile), 0) <= lax.rem(
        lax.broadcasted_iota(jnp.int32, (span, tile), 1), span
    )
    ones = jnp.ones((EXTRA, span), jnp.bfloat16)
    wide_v[head_size:tall, :] = jnp.ones_like(wide_v[head_size:tall, :])

    def group(blocks, first=False, final=False):
        high_masks, x_units = [], []

        def add_high(keys, masked):
            keys_h[nth(len(high_masks)), :] = keys
            high_masks.append(masked)

        def add_x(keys, is_low, masked):
            keys_x[nth(len(x_units)), :] = keys
            x_units.append((is_low, masked))

        def values_high(j, values):
            wide_v[:head_size, nth(j)] = values.T

        def values_x(j, values):
            is_low = x_units[j][0]
            at_j = nth(j)
            turned = values.T
            nil, none = jnp.zeros_like(turned), jnp.zeros_like(ones)
            if is_low is True:
                parts = (turned, ones, nil, none)
            else:
                parts = (
                    jnp.where(is_low, turned, nil),
                    jnp.where(is_low, ones, none),
                    jnp.where(is_low, nil, turned),
                    jnp.where(is_low, none, ones),
                )
            wide_v[tall : tall + head_size, at_j] = parts[0]
            wide_v[tall + head_size : 2 * tall, at_j] = parts[1]
            wide_v[2 * tall : 2 * tall + head_size, at_j] = parts[2]
            wide_v[2 * tall + head_size :, at_j] = parts[3]

        if first:
            k_low, k_high = halves_of(me, 0, swapped)
            add_high(k_low, False)
            add_high(k_high, True)
            add_x(k_low, True, True)
        for d in blocks:
            q, flip = pair_of(d)
            is_low = q < p
            k_low, k_high = halves_of(d, 0, flip)
            add_high(k_low, False)
            add_x(jnp.where(is_low, k_low, k_high), is_low, False)

        def turn_values():
            high, x = 0, 0
            if first:
                v_low, v_high = halves_of(me, 1, swapped)
                values_high(0, v_low)
                values_high(1, v_high)
                values_x(0, v_low)
                high, x = 2, 1
            for j, d in enumerate(blocks):
                v_low, v_high = halves_of(d, 1, pair_of(d)[1])
                values_high(high + j, v_low)
                values_x(x + j, jnp.where(x_units[x + j][0], v_low, v_high))

        turn_values()
        n_high, n_x = len(high_masks), len(x_units)
        units = n_high + n_x

        def base(t):
            return t * units if final else (t % 2) * 8

        def weights_at(t, of_x):
            if final:
                return t, of_x * n_high * span
            return (t % 2) * 2 + of_x, 0

        peaks = {}

        def start_tile(t):
            lt = lane_tile(t)
            if first:
                low = high = jnp.full((8, tile), NEG, jnp.float32)
            else:
                high, low = top[HIGH, :, lt], top[LOW, :, lt]
            peaks[t] = [high, low, high, low]

        def score_steps(t):
            lt = lane_tile(t)

            def of_high(lo, hi):
                found = jnp.dot(
                    keys_h[lo * span : hi * span, :], qt[HIGH, :, lt], preferred_element_type=jnp.float32
                )
                for u in range(lo, hi):
                    s = found[nth(u - lo)]
                    if high_masks[u]:
                        s = jnp.where(kept, s, NEG)
                    raw[base(t) + u] = s
                    peaks[t][2] = jnp.maximum(peaks[t][2], peak(s))

            def of_x(u):
                is_low, masked = x_units[u]
                which = LOW if is_low is True else 1 - is_low.astype(jnp.int32)
                s = jnp.dot(keys_x[nth(u), :], qt[which, :, lt], preferred_element_type=jnp.float32)
                if masked:
                    s = jnp.where(kept, s, NEG)
                raw[base(t) + n_high + u] = s
                m = peak(s)
                if is_low is True:
                    peaks[t][3] = jnp.maximum(peaks[t][3], m)
                else:
                    peaks[t][3] = jnp.where(is_low, jnp.maximum(peaks[t][3], m), peaks[t][3])
                    peaks[t][2] = jnp.where(is_low, peaks[t][2], jnp.maximum(peaks[t][2], m))

            steps = [
                functools.partial(of_high, lo, min(lo + 2, n_high)) for lo in range(0, n_high, 2)
            ]
            return steps + [functools.partial(of_x, u) for u in range(n_x)]

        def end_tile(t):
            lt = lane_tile(t)
            peaks[t][2:] = [spread(peaks[t][2]), spread(peaks[t][3])]
            top[HIGH, :, lt] = peaks[t][2]
            top[LOW, :, lt] = peaks[t][3]

        def weigh_steps(t):
            def weigh(u):
                if u < n_high:
                    m, row = peaks[t][2], u
                else:
                    is_low = x_units[u - n_high][0]
                    m = peaks[t][3] if is_low is True else jnp.where(is_low, peaks[t][3], peaks[t][2])
                    row = u - n_high
                dest, start = weights_at(t, int(u >= n_high))
                s = raw[base(t) + u].reshape(span // 8, 8, tile)
                w = jnp.exp2((s - m[None]) * factor)
                part[dest, start + row * span : start + (row + 1) * span, :] = w.reshape(span, tile).astype(jnp.bfloat16)

            return [functools.partial(weigh, u) for u in range(units)]

        def gather_values(t):
            lt = lane_tile(t)
            a, a0 = weights_at(t, 0)
            b, b0 = weights_at(t, 1)
            more = jnp.dot(
                wide_v[:tall, : n_high * span],
                part[a, a0 : a0 + n_high * span, :],
                preferred_element_type=jnp.float32,
            )
            both_rows = jnp.dot(
                wide_v[tall:, : n_x * span],
                part[b, b0 : b0 + n_x * span, :],
                preferred_element_type=jnp.float32,
            )
            if first:
                acc[HIGH, :, lt] = more + both_rows[tall:]
                acc[LOW, :, lt] = both_rows[:tall]
                return

            def scaled(which, old, new):
                shrink = jnp.exp2((old - new) * factor)
                return (acc[which, :, lt].reshape(tall // 8, 8, tile) * shrink[None]).reshape(tall, tile)

            high = scaled(HIGH, peaks[t][0], peaks[t][2]) + (more + both_rows[tall:])
            low = scaled(LOW, peaks[t][1], peaks[t][3]) + both_rows[:tall]
            if not final:
                acc[HIGH, :, lt] = high
                acc[LOW, :, lt] = low
                return
            rows_of = []
            for whole in (low, high):
                total = jnp.float32(1.0) / whole[head_size : head_size + 8]
                share = whole[:head_size].reshape(head_size // 8, 8, tile) * total[None]
                rows_of.append(share.reshape(head_size, tile).astype(jnp.bfloat16))
            for k in range(tile // span):
                low_rows, high_rows = (one[:, nth(k)].T for one in rows_of)
                cols = slice((t * (tile // span) + k) * head_size, (t * (tile // span) + k + 1) * head_size)
                out_ref[spans[0], cols] = jnp.where(swapped, high_rows, low_rows)
                out_ref[spans[1], cols] = jnp.where(swapped, low_rows, high_rows)

        start_tile(0)
        for step in score_steps(0):
            step()
        end_tile(0)
        for t in range(tiles):
            ahead = []
            if t + 1 < tiles:
                start_tile(t + 1)
                ahead = score_steps(t + 1)
            now = weigh_steps(t)
            for k in range(max(len(ahead), len(now))):
                if k < len(ahead):
                    ahead[k]()
                if k < len(now):
                    now[k]()
            if not final:
                gather_values(t)
            if t + 1 < tiles:
                end_tile(t + 1)
        if final:
            for t in range(tiles):
                gather_values(t)

    def run(todo):
        for one in todo:
            one()

    def mixed(a, b):
        return [one for pair in zip(a, b) for one in pair]

    def pair(r, yy):
        from_twin(plane(r), yy)
        return [at(plane(r), yy, c), at(plane(r), yy, 1 - c)]

    from_twin(z, y)
    group([twin], first=True)
    run(mixed(events(line_event, 1), events(side_event, 0)))
    for r in range(zs - 1):
        group(pair(r, far_y) + pair(r + 1, y))
        if r + 2 < zs:
            run(mixed(events(line_event, r + 2), events(side_event, r + 1)))
        else:
            run(events(side_event, r + 1))
    group(pair(zs - 1, far_y), final=True)
    all_sent()


def fused(n, queries, keys, values, span_order):
    local_rows, width = queries.shape
    head_size = keys.shape[1]
    heads = width // head_size
    span = local_rows // 2
    rows = heads * span
    anywhere = pl.BlockSpec(memory_space=pltpu.HBM)
    tall = head_size + EXTRA
    vmem = pl.BlockSpec(memory_space=pltpu.VMEM)
    return pl.pallas_call(
        functools.partial(fused_kernel, n, heads, span),
        out_shape=jax.ShapeDtypeStruct((local_rows, width), jnp.bfloat16),
        in_specs=[anywhere, anywhere, anywhere, anywhere],
        out_specs=vmem,
        scratch_shapes=[
            pltpu.SMEM(span_order.shape, jnp.int32),
            pltpu.VMEM((n, 2, local_rows, head_size), jnp.bfloat16),
            pltpu.VMEM((local_rows, width), jnp.bfloat16),
            pltpu.VMEM((2, head_size, rows), jnp.bfloat16),
            pltpu.VMEM((2, tall, rows), jnp.float32),
            pltpu.VMEM((2, 8, rows), jnp.float32),
            pltpu.VMEM((16, span, 2 * span), jnp.float32),
            pltpu.VMEM((4, 4 * span, 2 * span), jnp.bfloat16),
            pltpu.VMEM((3 * tall, 4 * span), jnp.bfloat16),
            pltpu.VMEM((4 * span, head_size), jnp.bfloat16),
            pltpu.VMEM((4 * span, head_size), jnp.bfloat16),
            pltpu.SemaphoreType.DMA((4,)),
            pltpu.SemaphoreType.DMA((1,)),
            pltpu.SemaphoreType.DMA((n // 4, 2, PIECES)),
            pltpu.SemaphoreType.DMA((n // 4, 2, PIECES)),
            pltpu.SemaphoreType.DMA((n // 4, 2)),
        ],
        compiler_params=pltpu.CompilerParams(
            collective_id=0, has_side_effects=True, vmem_limit_bytes=GRANT
        ),
        name="fused",
    )(*(pltpu.with_memory_space_constraint(x, pltpu.HBM) for x in (span_order, queries, keys, values)))


def body(n, queries, keys, values, span_order):
    if n <= FUSED_MOST:
        return fused(n, queries, keys, values, span_order)
    local_rows, width = queries.shape
    head_size = keys.shape[1]
    heads = width // head_size
    span = local_rows // 2
    vmem = pl.BlockSpec(memory_space=pltpu.VMEM)
    gathered = pl.pallas_call(
        functools.partial(gather_kernel, n),
        out_shape=jax.ShapeDtypeStruct((n, 2, local_rows, head_size), jnp.bfloat16),
        in_specs=[vmem, vmem],
        out_specs=vmem,
        scratch_shapes=[
            pltpu.SemaphoreType.DMA((n, 2, 4)),
            pltpu.SemaphoreType.DMA((n, 2)),
        ],
        compiler_params=pltpu.CompilerParams(collective_id=0, has_side_effects=True),
        name="gather",
    )(keys, values)
    half_keys = n * span
    more_keys = (n + 2) * span
    return pl.pallas_call(
        functools.partial(attend_kernel, n, heads, span),
        out_shape=jax.ShapeDtypeStruct((local_rows, width), jnp.bfloat16),
        in_specs=[vmem, vmem, pl.BlockSpec(memory_space=pltpu.SMEM)],
        out_specs=vmem,
        scratch_shapes=[
            pltpu.VMEM((2, heads, span, head_size), jnp.bfloat16),
            pltpu.VMEM((half_keys, head_size), jnp.bfloat16),
            pltpu.VMEM((half_keys, 2 * head_size), jnp.bfloat16),
            pltpu.VMEM((more_keys, head_size), jnp.bfloat16),
            pltpu.VMEM((more_keys, 2 * head_size), jnp.bfloat16),
            pltpu.VMEM((2, span, half_keys), jnp.float32),
            pltpu.VMEM((2, span, more_keys), jnp.float32),
            pltpu.VMEM((2, span, half_keys), jnp.bfloat16),
            pltpu.VMEM((2, span, more_keys), jnp.bfloat16),
        ],
        name="attend",
    )(queries, gathered, span_order)


def solution(mesh):
    in_specs = (
        P(("groups", "ctx"), None),
        P(("groups", "ctx"), None),
        P(("groups", "ctx"), None),
        P("groups"),
    )
    out_specs = P(("groups", "ctx"), None)
    return jax.shard_map(
        functools.partial(body, mesh.shape["ctx"]),
        mesh=mesh,
        in_specs=in_specs,
        out_specs=out_specs,
        check_vma=False,
    )
```
